16 devices in a mesh: dp: 2 (over z), stage: 2 (over y), tp: 4 (over x, core).
Axes of the slice: x: 2, y: 2, z: 2, core: 2. Of those that a mesh axis runs over, the one named last changes fastest.
Arguments:
- act_in: bfloat16 [2, 16, 28, 28, 512], P('stage', ('dp', 'tp'))
- conv_w: bfloat16 [2, 3, 3, 512, 1024], P('stage', None, None, 'tp')
- scale_vec: float32 [2, 1024], P('stage', 'tp')
- shift_vec: float32 [2, 1024], P('stage', 'tp')
- grad_z: bfloat16 [2, 16, 28, 28, 1024], P('stage', 'dp', None, None, 'tp')
Outputs:
- output 1: bfloat16 [2, 16, 28, 28, 1024], P('stage', 'dp', None, None, 'tp')
- output 2: bfloat16 [2, 16, 28, 28, 512], P('stage', ('dp', 'tp'))
- output 3: float32 [2, 3, 3, 512, 1024], P('stage', None, None, 'tp')
All inputs are finite; a program needn't handle non-finite values.
Results may differ from the reference program's by a relative error of at most 0.00419.
Values are sent between devices in bfloat16 or wider.
A program may use at most 1 GiB of HBM per device.

```python
import jax
import jax.numpy as jnp
from jax import lax

STAGES = 2
BATCH = 16
H = 28
W = 28
C = 512
CO = 1024


def place_stage(values, stage_index):
    pad_spec = [(stage_index, STAGES - 1 - stage_index)] + [(0, 0)] * values.ndim
    return jnp.pad(values[None], pad_spec)


def setup_inputs(seed: int = 0) -> dict:
    key = jax.random.key(seed)
    k_act, k_w, k_scale, k_sign, k_shift, k_grad = jax.random.split(key, 6)
    act_used = jax.random.normal(k_act, (BATCH, H, W, C), jnp.float32)
    w_used = jax.random.normal(k_w, (3, 3, C, CO), jnp.float32) * (9.0 * C) ** -0.5
    scale_sign = jnp.where(jax.random.randint(k_sign, (CO,), 0, 2) == 0, -1.0, 1.0)
    scale_used = scale_sign * jax.random.uniform(k_scale, (CO,), jnp.float32, 0.25, 1.75)
    shift_used = 0.8 * jax.random.normal(k_shift, (CO,), jnp.float32)
    grad_used = jax.random.normal(k_grad, (BATCH, H, W, CO), jnp.float32)
    return {
        "act_in": place_stage(act_used, 0).astype(jnp.bfloat16),
        "conv_w": place_stage(w_used, 1).astype(jnp.bfloat16),
        "scale_vec": place_stage(scale_used, 1),
        "shift_vec": place_stage(shift_used, 1),
        "grad_z": place_stage(grad_used, 1).astype(jnp.bfloat16),
    }


def conv_forward(images, kernel):
    return lax.conv_general_dilated(images, kernel, (1, 1), "SAME", dimension_numbers=("NHWC", "HWIO", "NHWC"))


def reference(act_in, conv_w, scale_vec, shift_vec, grad_z):
    kernel = conv_w[1].astype(jnp.float32)
    scale_one = scale_vec[1]
    shift_one = shift_vec[1]

    def one_image(dw_acc, img_pair):
        act_img, grad_img = img_pair
        image_f32 = act_img[None].astype(jnp.float32)
        pre_out, pull_back = jax.vjp(conv_forward, image_f32, kernel)
        lin_out = pre_out * scale_one + shift_one
        z_img = jnp.maximum(lin_out, 0.0).astype(jnp.bfloat16)
        grad_out = jnp.where(lin_out > 0, grad_img[None].astype(jnp.float32) * scale_one, 0.0).astype(jnp.bfloat16)
        dact_img, dw_img = pull_back(grad_out.astype(jnp.float32))
        return dw_acc + dw_img, (z_img[0], dact_img[0].astype(jnp.bfloat16))

    dw_init = jnp.zeros((3, 3, C, CO), jnp.float32)
    dw_sum, (z_used, dact_used) = lax.scan(one_image, dw_init, (act_in[0], grad_z[1]))
    return place_stage(z_used, 1), place_stage(dact_used, 0), place_stage(dw_sum, 1)
```

```python
import jax
import jax.numpy as jnp
from jax import lax
from jax.sharding import PartitionSpec as P


def conv_forward(images, kernel):
    return lax.conv_general_dilated(images, kernel, (1, 1), "SAME", dimension_numbers=("NHWC", "HWIO", "NHWC"), preferred_element_type=jnp.float32)


def conv_input_grad(grad_out, kernel):
    return lax.conv_general_dilated(grad_out, kernel[::-1, ::-1], (1, 1), "SAME", dimension_numbers=("NHWC", "HWOI", "NHWC"), preferred_element_type=jnp.float32)


def conv_kernel_grad(images, grad_out):
    return lax.conv_general_dilated(images, grad_out, (1, 1), ((1, 1), (1, 1)), dimension_numbers=("CHWN", "IHWO", "HWNC"), preferred_element_type=jnp.float32)


def solution(mesh):
    def body(act_loc, w_loc, scale_loc, shift_loc, grad_loc):
        kernel = w_loc[0]
        kern_out = lax.all_to_all(kernel, "tp", 3, 2, tiled=True)
        moved = lax.ppermute(act_loc[0], "stage", perm=[(0, 1)])
        act_all = lax.all_gather(moved, "tp", axis=0, tiled=True)
        pre_out = conv_forward(act_all, kern_out)
        lin_out = pre_out * scale_loc[0] + shift_loc[0]
        z_blk = jnp.maximum(lin_out, 0.0).astype(jnp.bfloat16)
        grad_blk = jnp.where(lin_out > 0, grad_loc[0].astype(jnp.float32) * scale_loc[0], 0.0).astype(jnp.bfloat16)
        grad_full = lax.all_gather(grad_blk, "tp", axis=3, tiled=True)
        tp_idx = lax.axis_index("tp")
        act_blk = lax.dynamic_slice_in_dim(act_all, tp_idx * 128, 128, axis=3)
        dw_part = conv_kernel_grad(act_blk, grad_full)
        dw_blk = lax.psum(dw_part, "dp")
        dact_blk = conv_input_grad(grad_full, kernel).astype(jnp.bfloat16)
        dact_back = lax.ppermute(dact_blk, "stage", perm=[(1, 0)])
        dact_img = lax.all_to_all(dact_back, "tp", 0, 3, tiled=True)
        return z_blk[None], dact_img[None], dw_blk[None]

    act_spec = P("stage", ("dp", "tp"))
    w_spec = P("stage", None, None, "tp")
    vec_spec = P("stage", "tp")
    grad_spec = P("stage", "dp", None, None, "tp")
    return jax.shard_map(body, mesh=mesh, in_specs=(act_spec, w_spec, vec_spec, vec_spec, grad_spec), out_specs=(grad_spec, act_spec, w_spec), check_vma=False)
```

```python
import functools

import jax
import jax.numpy as jnp
from jax import lax
from jax.experimental import pallas as pl
from jax.experimental.pallas import tpu as pltpu
from jax.sharding import PartitionSpec as P

BF = jnp.bfloat16
F32 = jnp.float32
MESH = pl.DeviceIdType.MESH
CH = 4
CR = 7


def kernel(act, w, sc, sh, gz, z_out, da_out, dw_out, A, AC, KO, KCU, KT, DZ, GU, W, WR, ACC, DAO, ZB,
           lsem, ksem_s, ksem_r, kc_s, kc_r, kc_l, as_s, a_r, f_s, g_s, g_r, zx_s, zx_r, da_s, da_r, out_s):
    dp = lax.axis_index("dp")
    stage = lax.axis_index("stage")
    t = lax.axis_index("tp")
    x = t // 2
    k = t % 2
    sib = x * 2 + (1 - k)
    xn = (1 - x) * 2 + k
    dg = (1 - x) * 2 + (1 - k)
    base = (1 - x) * 512

    def al(v, m):
        return pl.multiple_of(v, m)

    def remote(src, dst, ssem, rsem, **dev):
        return pltpu.make_async_remote_copy(src_ref=src, dst_ref=dst, send_sem=ssem, recv_sem=rsem, device_id=dev, device_id_type=MESH)

    A[0] = jnp.zeros((30, 8, 512), BF)
    A[29] = jnp.zeros((30, 8, 512), BF)
    A[:, 0] = jnp.zeros((30, 8, 512), BF)
    A[:, 29] = jnp.zeros((30, 8, 512), BF)

    def zero_halo(u, carry):
        GU[u, 0] = jnp.zeros((30, 8, 256), BF)
        GU[u, 29] = jnp.zeros((30, 8, 256), BF)
        GU[u, :, 0] = jnp.zeros((30, 8, 256), BF)
        GU[u, :, 29] = jnp.zeros((30, 8, 256), BF)
        return carry

    lax.fori_loop(0, 4, zero_halo, 0)

    barrier = pltpu.get_barrier_semaphore()
    for ds in range(2):
        for dt in range(4):
            if ds or dt:
                pl.semaphore_signal(barrier, inc=1, device_id={"stage": (stage + ds) % 2, "tp": (t + dt) % 4}, device_id_type=MESH)
    pl.semaphore_signal(barrier, inc=1, device_id={"dp": 1 - dp}, device_id_type=MESH)
    pl.semaphore_wait(barrier, 8)

    def k_copy(rel, peer, src_tp):
        return remote(w.at[:, :, pl.ds(al(256 * peer, 256), 256)], KO.at[:, pl.ds(al(128 * src_tp, 128), 128), :],
                      ksem_s.at[rel], ksem_r.at[rel], tp=peer)

    def kc_pieces(own, other):
        return ((0, 0, 256, 256 * own), (1, 0, 256, 256 * other), (2, 0, 128, base), (2, 128, 128, base + 256),
                (3, 0, 128, base + 128), (3, 128, 128, base + 384))

    def a_slot(src, c):
        return A.at[pl.ds(1 + CR * c, CR), pl.ds(1, 28), pl.ds(2 * src, 2), :]

    def a_direct(c):
        return remote(act.at[pl.ds(CR * c, CR)], a_slot(t, c), as_s.at[c], a_r.at[3, c], stage=1)

    def a_fwd(kind, c):
        if kind == 0:
            return remote(a_slot(t, c), a_slot(t, c), f_s.at[0, c], a_r.at[0, c], tp=sib)
        if kind == 1:
            return remote(a_slot(t, c), a_slot(t, c), f_s.at[1, c], a_r.at[1, c], tp=xn)
        return remote(a_slot(xn, c), a_slot(xn, c), f_s.at[2, c], a_r.at[2, c], tp=sib)

    def a_recv(rel, src, c):
        return remote(a_slot(src, c), a_slot(src, c), f_s.at[0, c], a_r.at[rel, c], tp=sib)

    def g_inner(u, lane, width):
        return GU.at[u, pl.ds(1, 28), pl.ds(1, 28), :, pl.ds(lane, width)]

    def da_copy(s, n):
        return remote(DAO.at[pl.ds(2 * n, 2), :, pl.ds(2 * s, 2), :],
                      da_out.at[pl.ds(14 * k + 2 * n, 2), :, :, pl.ds(al(256 * x, 256), 256)],
                      da_s.at[s, n], da_r.at[t, n], stage=0, tp=s)

    @pl.when(stage == 0)
    def _():
        for c in range(CH):
            a_direct(c).start()
        W[0] = jnp.zeros((9, 128, 256), F32)

        def zrow(h, carry):
            DZ[h] = jnp.zeros((28, 8, 256), BF)
            return carry

        lax.fori_loop(0, 28, zrow, 0)
        outs = [pltpu.make_async_copy(W.at[0], dw_out.at[:, :, pl.ds(256 * u, 256)], out_s.at[u]) for u in range(4)]
        outs.append(pltpu.make_async_copy(DZ, z_out, out_s.at[4]))
        for o in outs:
            o.start()
        for o in outs:
            o.wait()
        for c in range(CH):
            a_direct(c).wait_send()
        for src in range(4):
            for n in range(7):
                remote(DAO.at[pl.ds(2 * n, 2), :, pl.ds(0, 2), :],
                       da_out.at[pl.ds(14 * (src % 2) + 2 * n, 2), :, :, pl.ds(256 * (src // 2), 256)],
                       da_s.at[0, n], da_r.at[src, n], stage=0, tp=0).wait_recv()

    @pl.when(stage == 1)
    def _():
        k_copy(1, xn, t).start()
        k_copy(2, dg, t).start()
        k_copy(0, sib, t).start()
        for i, (u, lane, wd, src) in enumerate(kc_pieces(sib, t)):
            remote(w.at[:, :, pl.ds(al(src, 128), wd)], KCU.at[u, :, pl.ds(al(128 * k, 128), 128), pl.ds(lane, wd)],
                   kc_s.at[i], kc_r.at[i], tp=sib).start()
        loc = [pltpu.make_async_copy(w.at[:, :, pl.ds(al(src, 128), wd)], KCU.at[u, :, pl.ds(al(128 * k, 128), 128), pl.ds(lane, wd)], kc_l.at[i])
               for i, (u, lane, wd, src) in enumerate(kc_pieces(t, sib))]
        loc.append(pltpu.make_async_copy(w.at[:, :, pl.ds(al(256 * t, 256), 256)], KO.at[:, pl.ds(al(128 * t, 128), 128), :], lsem.at[0]))
        loc.append(pltpu.make_async_copy(gz, DZ, lsem.at[1]))
        for o in loc:
            o.start()
        ZB[...] = jnp.zeros((7, 28, 2, 512), BF)
        zcp = [pltpu.make_async_copy(ZB, da_out.at[pl.ds(7 * i, 7)], out_s.at[i]) for i in range(4)]
        for o in zcp:
            o.start()
        ACC[...] = jnp.zeros((14, 224, 256), F32)

        for c in range(CH):
            a_recv(3, t, c).wait_recv()
            a_fwd(1, c).start()
            a_fwd(0, c).start()
            if c == 0:
                for o in loc:
                    o.wait()
                for o in zcp:
                    o.wait()
                for i, (u, lane, wd, src) in enumerate(kc_pieces(t, sib)):
                    remote(w.at[:, :, pl.ds(al(src, 128), wd)], KCU.at[u, :, pl.ds(al(128 * (1 - k), 128), 128), pl.ds(lane, wd)],
                           kc_s.at[i], kc_r.at[i], tp=sib).wait_recv()

            def tr(tap, carry, c=c):
                KT[c, pl.ds(tap * 256, 256)] = KCU[c, tap].T
                return carry

            lax.fori_loop(0, 9, tr, 0)

        k_copy(1, t, xn).wait_recv()
        k_copy(2, t, dg).wait_recv()
        k_copy(0, t, sib).wait_recv()

        def chunk(c, carry):
            a_recv(1, xn, c).wait_recv()
            a_fwd(2, c).start()
            a_recv(0, sib, c).wait_recv()
            a_recv(2, dg, c).wait_recv()

            def row(h, inner):
                lhs = jnp.concatenate([A[h + i, j:j + 28].reshape(224, 512) for i in range(3) for j in range(3)], axis=1)
                pre = jnp.dot(lhs, KO[...].reshape(4608, 256), preferred_element_type=F32)
                y = pre * sc[...] + sh[...]
                d = DZ[h].reshape(224, 256).astype(F32)
                g = jnp.where(y > 0, d * sc[...], 0.0).astype(BF)
                DZ[h] = jnp.maximum(y, 0.0).astype(BF).reshape(28, 8, 256)
                GU[0, h + 1, 1:29] = g.reshape(28, 8, 256)
                return inner

            lax.fori_loop(CR * c - (c + 2) // 3, CR * (c + 1) - 1 + c // 3, row, 0)
            return carry

        lax.fori_loop(0, CH, chunk, 0)

        z_cp = pltpu.make_async_copy(DZ, z_out, lsem.at[0])
        ac_cp = pltpu.make_async_copy(A.at[:, :, :, pl.ds(al(128 * t, 128), 128)], AC, lsem.at[1])
        g_sib = remote(GU.at[0], GU.at[1], g_s.at[0], g_r.at[0], tp=sib)
        g_x = [remote(g_inner(0, 128 * q, 128), g_inner(2 + q, al(128 * k, 128), 128), g_s.at[1 + q], g_r.at[1 + q], tp=xn) for q in range(2)]
        g_rel = [remote(g_inner(2 + q, al(128 * k, 128), 128), g_inner(2 + q, al(128 * k, 128), 128), g_s.at[3 + q], g_r.at[3 + q], tp=sib) for q in range(2)]
        ac_cp.start()
        g_x[0].start()
        g_x[1].start()
        g_sib.start()
        z_cp.start()
        ac_cp.wait()

        zx = [remote(W.at[u], WR.at[u], zx_s.at[u], zx_r.at[u], dp=1 - dp) for u in range(4)]

        def dw_unit(u):
            W[u] = jnp.zeros((9, 128, 256), F32)

            def step(n, carry):
                h = n * 7
                lhs = jnp.concatenate([AC[pl.ds(h + i, 7), j:j + 28].reshape(1568, 128) for i in range(3) for j in range(3)], axis=1)
                rhs = GU[u, pl.ds(h + 1, 7), 1:29].reshape(1568, 256)
                p = lax.dot_general(lhs, rhs, (((0,), (0,)), ((), ())), preferred_element_type=F32)
                W[u] += p.reshape(9, 128, 256)
                return carry

            lax.fori_loop(0, 4, step, 0)
            zx[u].start()

        def da_rows(u, n):
            h = 14 * k + 2 * n
            lhs = jnp.concatenate([GU[u, pl.ds(h + 2 - i, 2), 2 - j:30 - j].reshape(448, 256) for i in range(3) for j in range(3)], axis=1)
            return jnp.dot(lhs, KT[u], preferred_element_type=F32)

        def da_unit(u):
            def step(n, carry):
                ACC[pl.ds(2 * n, 2)] += da_rows(u, n).reshape(2, 224, 256)
                return carry

            lax.fori_loop(0, 7, step, 0)

        dw_dst = ((256 * t,), (256 * sib,), (base, base + 256), (base + 128, base + 384))

        def dw_out_cp(u):
            starts = dw_dst[u]
            wd = 256 // len(starts)
            return [pltpu.make_async_copy(WR.at[u, :, :, pl.ds(wd * i, wd)], dw_out.at[:, :, pl.ds(al(s, 128), wd)], kc_l.at[2 * (u // 2) + (u % 2) * (u // 2) + u % 2 + i])
                    for i, s in enumerate(starts)]

        def dw_final(u):
            zx[u].wait_recv()

            def add(q, carry):
                WR[u, q] += W[u, q]
                return carry

            lax.fori_loop(0, 9, add, 0)
            for o in dw_out_cp(u):
                o.start()

        dw_unit(0)
        g_sib.wait_recv()
        dw_unit(1)
        da_unit(0)
        da_unit(1)
        for q in range(2):
            u = 2 + q
            g_x[q].wait_recv()
            g_rel[q].start()
            remote(g_inner(u, 0, 128), g_inner(u, al(128 * (1 - k), 128), 128), g_s.at[3 + q], g_r.at[3 + q], tp=sib).wait_recv()
            dw_unit(u)
            if q == 0:
                da_unit(2)
                dw_final(0)

        def last(n, carry):
            v = ACC[pl.ds(2 * n, 2)].reshape(448, 256) + da_rows(3, n)
            DAO[pl.ds(2 * n, 2)] = v.astype(BF).reshape(2, 28, 8, 256)
            for s in range(4):
                da_copy(s, n).start()
            return carry

        lax.fori_loop(0, 7, last, 0)
        for u in range(1, 4):
            dw_final(u)

        z_cp.wait()
        for u in range(4):
            for o in dw_out_cp(u):
                o.wait()
            zx[u].wait_send()
        k_copy(1, xn, t).wait_send()
        k_copy(2, dg, t).wait_send()
        k_copy(0, sib, t).wait_send()
        for i, (u, lane, wd, src) in enumerate(kc_pieces(sib, t)):
            remote(w.at[:, :, pl.ds(al(src, 128), wd)], KCU.at[u, :, pl.ds(al(128 * k, 128), 128), pl.ds(lane, wd)],
                   kc_s.at[i], kc_r.at[i], tp=sib).wait_send()
        for c in range(CH):
            for kind in range(3):
                a_fwd(kind, c).wait_send()
        g_sib.wait_send()
        for q in range(2):
            g_x[q].wait_send()
            g_rel[q].wait_send()
        for s in range(4):
            for n in range(7):
                da_copy(s, n).wait_send()


def solution(mesh):
    V = pltpu.VMEM
    D = pltpu.SemaphoreType.DMA
    any_spec = pl.BlockSpec(memory_space=pl.ANY)
    vm_spec = pl.BlockSpec(memory_space=pltpu.VMEM)
    call = pl.pallas_call(
        kernel,
        out_shape=[jax.ShapeDtypeStruct((28, 28, 8, 256), BF), jax.ShapeDtypeStruct((28, 28, 2, 512), BF), jax.ShapeDtypeStruct((9, 128, 1024), F32)],
        in_specs=[any_spec, any_spec, vm_spec, vm_spec, any_spec],
        out_specs=[any_spec] * 3,
        scratch_shapes=[
            V((30, 30, 8, 512), BF), V((30, 30, 8, 128), BF), V((9, 512, 256), BF), V((4, 9, 256, 256), BF), V((4, 2304, 256), BF),
            V((28, 28, 8, 256), BF), V((4, 30, 30, 8, 256), BF), V((4, 9, 128, 256), F32), V((4, 9, 128, 256), F32),
            V((14, 224, 256), F32), V((14, 28, 8, 256), BF), V((7, 28, 2, 512), BF),
            D((2,)), D((3,)), D((3,)), D((6,)), D((6,)), D((6,)), D((4,)), D((4, 4)), D((3, 4)), D((5,)), D((5,)), D((4,)), D((4,)),
            D((4, 7)), D((4, 7)), D((5,)),
        ],
        compiler_params=pltpu.CompilerParams(collective_id=0, has_side_effects=True, vmem_limit_bytes=66000000),
        name="conv_block",
    )

    def body(act_loc, w_loc, scale_loc, shift_loc, grad_loc):
        z, da, dw = call(act_loc[0].transpose(1, 2, 0, 3), w_loc[0].reshape(9, 128, 1024), scale_loc, shift_loc, grad_loc[0].transpose(1, 2, 0, 3))
        return z.transpose(2, 0, 1, 3)[None], da.transpose(2, 0, 1, 3)[None], dw.reshape(1, 3, 3, 128, 1024)

    act_spec = P("stage", ("dp", "tp"))
    w_spec = P("stage", None, None, "tp")
    vec_spec = P("stage", "tp")
    grad_spec = P("stage", "dp", None, None, "tp")
    return jax.shard_map(body, mesh=mesh, in_specs=(act_spec, w_spec, vec_spec, vec_spec, grad_spec), out_specs=(grad_spec, act_spec, w_spec), check_vma=False)
```

```python
import functools

import jax
import jax.numpy as jnp
from jax import lax
from jax.experimental import pallas as pl
from jax.experimental.pallas import tpu as pltpu
from jax.sharding import PartitionSpec as P

BF = jnp.bfloat16
F32 = jnp.float32
MESH = pl.DeviceIdType.MESH
CH = 4
CB = (0, 8, 15, 22, 28)
GP = ((0, 15), (15, 13))


def kernel(act, w, sc, sh, gz, z_out, da_out, dw_out, A, AC, KO, KCU, KT, DZ, GU, W, WR, ACC, DAO, ZB,
           lsem, ksem_s, ksem_r, kc_s, kc_r, kc_l, as_s, ax_r, a_r, f_s, gs_s, gs_r, g2_s, g2_r, g3_s, g3_r, rel_s, rel_r,
           zx_s, zx_r, d_s, d_r, da_s, da_r, out_s):
    dp = lax.axis_index("dp")
    stage = lax.axis_index("stage")
    t = lax.axis_index("tp")
    x = t // 2
    k = t % 2
    sib = x * 2 + (1 - k)
    xn = (1 - x) * 2 + k
    dg = (1 - x) * 2 + (1 - k)
    pz = (1 - x) * 2 + (k + dp) % 2
    pz2 = (1 - x) * 2 + (k + 1 - dp) % 2
    base = (1 - x) * 512

    def al(v, m):
        return pl.multiple_of(v, m)

    def remote(src, dst, ssem, rsem, **dev):
        return pltpu.make_async_remote_copy(src_ref=src, dst_ref=dst, send_sem=ssem, recv_sem=rsem, device_id=dev, device_id_type=MESH)

    A[0] = jnp.zeros((30, 8, 512), BF)
    A[29] = jnp.zeros((30, 8, 512), BF)
    A[:, 0] = jnp.zeros((30, 8, 512), BF)
    A[:, 29] = jnp.zeros((30, 8, 512), BF)

    def zero_halo(u, carry):
        GU[u, 0] = jnp.zeros((30, 8, 256), BF)
        GU[u, 29] = jnp.zeros((30, 8, 256), BF)
        GU[u, :, 0] = jnp.zeros((30, 8, 256), BF)
        GU[u, :, 29] = jnp.zeros((30, 8, 256), BF)
        return carry

    lax.fori_loop(0, 4, zero_halo, 0)

    barrier = pltpu.get_barrier_semaphore()
    for ds in range(2):
        for dt in range(4):
            if ds or dt:
                pl.semaphore_signal(barrier, inc=1, device_id={"stage": (stage + ds) % 2, "tp": (t + dt) % 4}, device_id_type=MESH)
    pl.semaphore_signal(barrier, inc=1, device_id={"dp": 1 - dp}, device_id_type=MESH)
    pl.semaphore_wait(barrier, 8)

    def k_slot(src_tp):
        return KO.at[:, pl.ds(al(128 * src_tp, 128), 128), :]

    def k_copy(rel, peer, src_tp):
        return remote(w.at[:, :, pl.ds(al(256 * peer, 256), 256)], k_slot(src_tp), ksem_s.at[rel], ksem_r.at[rel], tp=peer)

    def k_z(src_tp):
        return remote(k_slot(src_tp), k_slot(src_tp), ksem_s.at[2], ksem_r.at[2], dp=1 - dp)

    def kc_pieces(own, other):
        return ((0, 0, 256, 256 * own), (1, 0, 256, 256 * other), (2, 0, 128, base), (2, 128, 128, base + 256),
                (3, 0, 128, base + 128), (3, 128, 128, base + 384))

    def a_slot(src, c):
        return A.at[pl.ds(1 + CB[c], CB[c + 1] - CB[c]), pl.ds(1, 28), pl.ds(2 * src, 2), :]

    def a_direct(c):
        return remote(act.at[pl.ds(CB[c], CB[c + 1] - CB[c])], a_slot(t, c), as_s.at[c], a_r.at[3, c], stage=1)

    def a_cross():
        return remote(act.at[pl.ds(CB[3], CB[4] - CB[3])], a_slot(t, 3), as_s.at[4], ax_r.at[0], tp=xn)

    def a_cross_fwd():
        return remote(a_slot(xn, 3), a_slot(xn, 3), as_s.at[5], a_r.at[1, 3], stage=1)

    def a_fwd(kind, c):
        if kind == 0:
            return remote(a_slot(t, c), a_slot(t, c), f_s.at[0, c], a_r.at[0, c], tp=sib)
        if kind == 1:
            return remote(a_slot(t, c), a_slot(t, c), f_s.at[1, c], a_r.at[1, c], tp=xn)
        return remote(a_slot(xn, c), a_slot(xn, c), f_s.at[2, c], a_r.at[2, c], tp=sib)

    def a_recv(rel, src, c):
        return remote(a_slot(src, c), a_slot(src, c), f_s.at[0, c], a_r.at[rel, c], tp=sib)

    def g_rows(u, r0, n, lane, width):
        return GU.at[u, pl.ds(1 + r0, n), pl.ds(1, 28), :, pl.ds(lane, width)]

    mine = al(128 * k, 128)
    theirs = al(128 * (1 - k), 128)

    def g2(c):
        return remote(g_rows(0, 7 * c, 7, 0, 128), g_rows(2, 7 * c, 7, mine, 128), g2_s.at[c], g2_r.at[c], tp=xn)

    def g3(p):
        return remote(g_rows(0, GP[p][0], GP[p][1], 128, 128), g_rows(3, GP[p][0], GP[p][1], mine, 128), g3_s.at[p], g3_r.at[p], tp=xn)

    def g2_rel(lane):
        return remote(g_rows(2, 0, 28, lane, 128), g_rows(2, 0, 28, lane, 128), rel_s.at[0], rel_r.at[0], tp=sib)

    def g3_rel(p, lane):
        return remote(g_rows(3, GP[p][0], GP[p][1], lane, 128), g_rows(3, GP[p][0], GP[p][1], lane, 128), rel_s.at[1 + p], rel_r.at[1 + p], tp=sib)

    def det(leg, p):
        src, dst = ((W, WR), (WR, W), (W, WR))[leg]
        dev = ({"stage": 0}, {"dp": 1 - dp}, {"stage": 1})[leg]
        return remote(src.at[1, pl.ds(3 * p, 3)], dst.at[1, pl.ds(3 * p, 3)], d_s.at[leg, p], d_r.at[leg, p], **dev)

    def da_copy(s, n):
        return remote(DAO.at[pl.ds(2 * n, 2), :, pl.ds(2 * s, 2), :],
                      da_out.at[pl.ds(14 * k + 2 * n, 2), :, :, pl.ds(al(256 * x, 256), 256)],
                      da_s.at[s, n], da_r.at[t, n], stage=0, tp=s)

    @pl.when(stage == 0)
    def _():
        a_cross().start()
        for c in range(CH):
            a_direct(c).start()
        a_cross().wait_recv()
        a_cross_fwd().start()
        W[0] = jnp.zeros((9, 128, 256), F32)

        def zrow(h, carry):
            DZ[h] = jnp.zeros((28, 8, 256), BF)
            return carry

        lax.fori_loop(0, 28, zrow, 0)
        outs = [pltpu.make_async_copy(W.at[0], dw_out.at[:, :, pl.ds(256 * u, 256)], out_s.at[u]) for u in range(4)]
        outs.append(pltpu.make_async_copy(DZ, z_out, out_s.at[4]))
        for o in outs:
            o.start()
        for o in outs:
            o.wait()
        for leg, p in ((0, 0), (0, 1), (1, 0), (0, 2), (1, 1), (1, 2)):
            det(leg, p).wait_recv()
            det(leg + 1, p).start()
        for c in range(CH):
            a_direct(c).wait_send()
        a_cross().wait_send()
        a_cross_fwd().wait_send()
        for p in range(3):
            det(1, p).wait_send()
            det(2, p).wait_send()
        for src in range(4):
            for n in range(7):
                remote(DAO.at[pl.ds(2 * n, 2), :, pl.ds(0, 2), :],
                       da_out.at[pl.ds(14 * (src % 2) + 2 * n, 2), :, :, pl.ds(256 * (src // 2), 256)],
                       da_s.at[0, n], da_r.at[src, n], stage=0, tp=0).wait_recv()

    @pl.when(stage == 1)
    def _():
        k_copy(1, pz, t).start()
        k_copy(0, sib, t).start()
        for i, (u, lane, wd, src) in enumerate(kc_pieces(sib, t)):
            remote(w.at[:, :, pl.ds(al(src, 128), wd)], KCU.at[u, :, pl.ds(al(128 * k, 128), 128), pl.ds(lane, wd)],
                   kc_s.at[i], kc_r.at[i], tp=sib).start()
        loc = [pltpu.make_async_copy(w.at[:, :, pl.ds(al(src, 128), wd)], KCU.at[u, :, pl.ds(al(128 * k, 128), 128), pl.ds(lane, wd)], kc_l.at[i])
               for i, (u, lane, wd, src) in enumerate(kc_pieces(t, sib))]
        loc.append(pltpu.make_async_copy(w.at[:, :, pl.ds(al(256 * t, 256), 256)], KO.at[:, pl.ds(al(128 * t, 128), 128), :], lsem.at[0]))
        loc.append(pltpu.make_async_copy(gz, DZ, lsem.at[1]))
        for o in loc:
            o.start()
        ZB[...] = jnp.zeros((7, 28, 2, 512), BF)
        zcp = [pltpu.make_async_copy(ZB, da_out.at[pl.ds(7 * i, 7)], out_s.at[i]) for i in range(4)]
        for o in zcp:
            o.start()
        ACC[...] = jnp.zeros((14, 224, 256), F32)

        for c in range(CH):
            a_recv(3, t, c).wait_recv()
            if c < 3:
                a_fwd(1, c).start()
            a_fwd(0, c).start()
            if c == 0:
                for o in loc:
                    o.wait()
                for o in zcp:
                    o.wait()
                for i, (u, lane, wd, src) in enumerate(kc_pieces(t, sib)):
                    remote(w.at[:, :, pl.ds(al(src, 128), wd)], KCU.at[u, :, pl.ds(al(128 * (1 - k), 128), 128), pl.ds(lane, wd)],
                           kc_s.at[i], kc_r.at[i], tp=sib).wait_recv()
            if c == 1:
                k_copy(1, t, pz).wait_recv()
                k_z(pz).start()

            def tr(tap, carry, c=c):
                KT[c, pl.ds(tap * 256, 256)] = KCU[c, tap].T
                return carry

            lax.fori_loop(0, 9, tr, 0)

        k_z(pz2).wait_recv()
        k_copy(0, t, sib).wait_recv()

        def row(h, carry):
            lhs = jnp.concatenate([A[h + i, j:j + 28].reshape(224, 512) for i in range(3) for j in range(3)], axis=1)
            pre = jnp.dot(lhs, KO[...].reshape(4608, 256), preferred_element_type=F32)
            y = pre * sc[...] + sh[...]
            d = DZ[h].reshape(224, 256).astype(F32)
            g = jnp.where(y > 0, d * sc[...], 0.0).astype(BF)
            DZ[h] = jnp.maximum(y, 0.0).astype(BF).reshape(28, 8, 256)
            GU[0, h + 1, 1:29] = g.reshape(28, 8, 256)
            return carry

        z_cp = pltpu.make_async_copy(DZ, z_out, lsem.at[0])
        ac_cp = pltpu.make_async_copy(A.at[:, :, :, pl.ds(al(128 * t, 128), 128)], AC, lsem.at[1])
        g_sib = remote(GU.at[0], GU.at[1], gs_s.at[0], gs_r.at[0], tp=sib)

        for c in range(CH):
            a_recv(1, xn, c).wait_recv()
            a_fwd(2, c).start()
            a_recv(0, sib, c).wait_recv()
            a_recv(2, dg, c).wait_recv()
            if c == CH - 1:
                ac_cp.start()
            lax.fori_loop(7 * c, 7 * c + 7, row, 0)
            g2(c).start()
        for p in range(2):
            g3(p).start()
        g_sib.start()
        z_cp.start()
        ac_cp.wait()

        zx = {u: remote(W.at[u], WR.at[u], zx_s.at[u], zx_r.at[u], dp=1 - dp) for u in (0, 2, 3)}

        def dw_unit(u):
            W[u] = jnp.zeros((9, 128, 256), F32)

            def step(n, carry):
                h = n * 7
                lhs = jnp.concatenate([AC[pl.ds(h + i, 7), j:j + 28].reshape(1568, 128) for i in range(3) for j in range(3)], axis=1)
                rhs = GU[u, pl.ds(h + 1, 7), 1:29].reshape(1568, 256)
                p = lax.dot_general(lhs, rhs, (((0,), (0,)), ((), ())), preferred_element_type=F32)
                W[u] += p.reshape(9, 128, 256)
                return carry

            lax.fori_loop(0, 4, step, 0)
            if u == 1:
                for p in range(3):
                    det(0, p).start()
            else:
                zx[u].start()

        def da_rows(u, n):
            h = 14 * k + 2 * n
            lhs = jnp.concatenate([GU[u, pl.ds(h + 2 - i, 2), 2 - j:30 - j].reshape(448, 256) for i in range(3) for j in range(3)], axis=1)
            return jnp.dot(lhs, KT[u], preferred_element_type=F32)

        def da_unit(u):
            def step(n, carry):
                ACC[pl.ds(2 * n, 2)] += da_rows(u, n).reshape(2, 224, 256)
                return carry

            lax.fori_loop(0, 7, step, 0)

        dw_dst = ((256 * t,), (256 * sib,), (base, base + 256), (base + 128, base + 384))

        def dw_out_cp(u):
            starts = dw_dst[u]
            wd = 256 // len(starts)
            return [pltpu.make_async_copy(WR.at[u, :, :, pl.ds(wd * i, wd)], dw_out.at[:, :, pl.ds(al(s, 128), wd)], kc_l.at[2 * (u // 2) + (u % 2) * (u // 2) + u % 2 + i])
                    for i, s in enumerate(starts)]

        def dw_final(u):
            if u == 1:
                for p in range(3):
                    det(2, p).wait_recv()
            else:
                zx[u].wait_recv()

            def add(q, carry):
                WR[u, q] += W[u, q]
                return carry

            lax.fori_loop(0, 9, add, 0)
            for o in dw_out_cp(u):
                o.start()

        dw_unit(0)
        g_sib.wait_recv()
        dw_unit(1)
        da_unit(0)
        da_unit(1)
        def last(n, carry):
            v = ACC[pl.ds(2 * n, 2)].reshape(448, 256) + da_rows(3, n)
            DAO[pl.ds(2 * n, 2)] = v.astype(BF).reshape(2, 28, 8, 256)
            for s in range(4):
                da_copy(s, n).start()
            return carry

        for c in range(CH):
            g2(c).wait_recv()
        g2_rel(mine).start()
        g2_rel(theirs).wait_recv()
        dw_unit(2)
        da_unit(2)
        dw_final(0)
        g3(0).wait_recv()
        g3_rel(0, mine).start()
        g3_rel(0, theirs).wait_recv()

        @pl.when(k == 0)
        def _():
            lax.fori_loop(0, 7, last, 0)

        dw_final(1)
        g3(1).wait_recv()
        g3_rel(1, mine).start()
        g3_rel(1, theirs).wait_recv()
        dw_unit(3)

        @pl.when(k == 1)
        def _():
            lax.fori_loop(0, 7, last, 0)

        for u in range(2, 4):
            dw_final(u)

        z_cp.wait()
        for u in range(4):
            for o in dw_out_cp(u):
                o.wait()
            if u != 1:
                zx[u].wait_send()
        for p in range(3):
            det(0, p).wait_send()
        k_copy(1, pz, t).wait_send()
        k_z(pz).wait_send()
        k_copy(0, sib, t).wait_send()
        for i, (u, lane, wd, src) in enumerate(kc_pieces(sib, t)):
            remote(w.at[:, :, pl.ds(al(src, 128), wd)], KCU.at[u, :, pl.ds(al(128 * k, 128), 128), pl.ds(lane, wd)],
                   kc_s.at[i], kc_r.at[i], tp=sib).wait_send()
        for c in range(CH):
            for kind in range(3):
                if kind != 1 or c < 3:
                    a_fwd(kind, c).wait_send()
            g2(c).wait_send()
        g_sib.wait_send()
        g2_rel(mine).wait_send()
        for p in range(2):
            g3(p).wait_send()
            g3_rel(p, mine).wait_send()
        for s in range(4):
            for n in range(7):
                da_copy(s, n).wait_send()


def solution(mesh):
    V = pltpu.VMEM
    D = pltpu.SemaphoreType.DMA
    any_spec = pl.BlockSpec(memory_space=pl.ANY)
    vm_spec = pl.BlockSpec(memory_space=pltpu.VMEM)
    call = pl.pallas_call(
        kernel,
        out_shape=[jax.ShapeDtypeStruct((28, 28, 8, 256), BF), jax.ShapeDtypeStruct((28, 28, 2, 512), BF), jax.ShapeDtypeStruct((9, 128, 1024), F32)],
        in_specs=[any_spec, any_spec, vm_spec, vm_spec, any_spec],
        out_specs=[any_spec] * 3,
        scratch_shapes=[
            V((30, 30, 8, 512), BF), V((30, 30, 8, 128), BF), V((9, 512, 256), BF), V((4, 9, 256, 256), BF), V((4, 2304, 256), BF),
            V((28, 28, 8, 256), BF), V((4, 30, 30, 8, 256), BF), V((4, 9, 128, 256), F32), V((4, 9, 128, 256), F32),
            V((14, 224, 256), F32), V((14, 28, 8, 256), BF), V((7, 28, 2, 512), BF),
            D((2,)), D((3,)), D((3,)), D((6,)), D((6,)), D((6,)), D((6,)), D((1,)), D((4, 4)), D((3, 4)), D((1,)), D((1,)), D((4,)), D((4,)),
            D((2,)), D((2,)), D((3,)), D((3,)), D((4,)), D((4,)), D((3, 3)), D((3, 3)), D((4, 7)), D((4, 7)), D((5,)),
        ],
        compiler_params=pltpu.CompilerParams(collective_id=0, has_side_effects=True, vmem_limit_bytes=66000000),
        name="conv_block",
    )

    def body(act_loc, w_loc, scale_loc, shift_loc, grad_loc):
        z, da, dw = call(act_loc[0].transpose(1, 2, 0, 3), w_loc[0].reshape(9, 128, 1024), scale_loc, shift_loc, grad_loc[0].transpose(1, 2, 0, 3))
        return z.transpose(2, 0, 1, 3)[None], da.transpose(2, 0, 1, 3)[None], dw.reshape(1, 3, 3, 128, 1024)

    act_spec = P("stage", ("dp", "tp"))
    w_spec = P("stage", None, None, "tp")
    vec_spec = P("stage", "tp")
    grad_spec = P("stage", "dp", None, None, "tp")
    return jax.shard_map(body, mesh=mesh, in_specs=(act_spec, w_spec, vec_spec, vec_spec, grad_spec), out_specs=(grad_spec, act_spec, w_spec), check_vma=False)
```

```python
import functools

import jax
import jax.numpy as jnp
from jax import lax
from jax.experimental import pallas as pl
from jax.experimental.pallas import tpu as pltpu
from jax.sharding import PartitionSpec as P

BF = jnp.bfloat16
F32 = jnp.float32
MESH = pl.DeviceIdType.MESH
CH = 4
CB = (0, 8, 15, 22, 28)
GP = ((0, 8), (8, 7), (20, 8), (15, 5))
HW = 28
HP = 30
NB = 8
RW = 224
TAPS = 9
LN = 128
BLK = 256
CIN = 512


def kernel(act, w, sc, sh, gz, z_out, da_out, dw_out, A, AC, KO, KCU, KT, DZ, GU, W, WR, ACC, DAO, ZB,
           lsem, ksem_s, ksem_r, kc_s, kc_r, kc_l, as_s, ax_r, a_r, f_s, gs_s, gs_r, g2_s, g2_r, g3_s, g3_r, gd_s, gd_r, rel_s, rel_r,
           zx_s, zx_r, d_s, d_r, da_s, da_r, out_s):
    dp = lax.axis_index("dp")
    stage = lax.axis_index("stage")
    t = lax.axis_index("tp")
    x = t // 2
    k = t % 2
    sib = x * 2 + (1 - k)
    xn = (1 - x) * 2 + k
    dg = (1 - x) * 2 + (1 - k)
    pz = (1 - x) * 2 + (k + dp) % 2
    pz2 = (1 - x) * 2 + (k + 1 - dp) % 2
    base = (1 - x) * CIN

    def al(v, m):
        return pl.multiple_of(v, m)

    def remote(src, dst, ssem, rsem, **dev):
        return pltpu.make_async_remote_copy(src_ref=src, dst_ref=dst, send_sem=ssem, recv_sem=rsem, device_id=dev, device_id_type=MESH)

    A[0] = jnp.zeros((HP, NB, CIN), BF)
    A[29] = jnp.zeros((HP, NB, CIN), BF)
    A[:, 0] = jnp.zeros((HP, NB, CIN), BF)
    A[:, 29] = jnp.zeros((HP, NB, CIN), BF)

    def zero_halo(u, carry):
        GU[u, 0] = jnp.zeros((HP, NB, BLK), BF)
        GU[u, 29] = jnp.zeros((HP, NB, BLK), BF)
        GU[u, :, 0] = jnp.zeros((HP, NB, BLK), BF)
        GU[u, :, 29] = jnp.zeros((HP, NB, BLK), BF)
        return carry

    lax.fori_loop(0, 4, zero_halo, 0)

    barrier = pltpu.get_barrier_semaphore()
    for ds in range(2):
        for dt in range(4):
            if ds or dt:
                pl.semaphore_signal(barrier, inc=1, device_id={"stage": (stage + ds) % 2, "tp": (t + dt) % 4}, device_id_type=MESH)
    pl.semaphore_signal(barrier, inc=1, device_id={"dp": 1 - dp}, device_id_type=MESH)
    pl.semaphore_wait(barrier, NB)

    def k_slot(src_tp):
        return KO.at[:, pl.ds(al(LN * src_tp, LN), LN), :]

    def k_copy(rel, peer, src_tp):
        return remote(w.at[:, :, pl.ds(al(BLK * peer, BLK), BLK)], k_slot(src_tp), ksem_s.at[rel], ksem_r.at[rel], tp=peer)

    def k_z(src_tp):
        return remote(k_slot(src_tp), k_slot(src_tp), ksem_s.at[2], ksem_r.at[2], dp=1 - dp)

    def kc_pieces(own, other):
        return ((0, 0, BLK, BLK * own), (1, 0, BLK, BLK * other), (2, 0, LN, base), (2, LN, LN, base + BLK),
                (3, 0, LN, base + LN), (3, LN, LN, base + 384))

    def a_slot(src, c):
        return A.at[pl.ds(1 + CB[c], CB[c + 1] - CB[c]), pl.ds(1, HW), pl.ds(2 * src, 2), :]

    def a_direct(c):
        return remote(act.at[pl.ds(CB[c], CB[c + 1] - CB[c])], a_slot(t, c), as_s.at[c], a_r.at[3, c], stage=1)

    def a_cross():
        return remote(act.at[pl.ds(CB[3], CB[4] - CB[3])], a_slot(t, 3), as_s.at[4], ax_r.at[0], tp=xn)

    def a_cross_fwd():
        return remote(a_slot(xn, 3), a_slot(xn, 3), as_s.at[5], a_r.at[1, 3], stage=1)

    def a_fwd(kind, c):
        if kind == 0:
            return remote(a_slot(t, c), a_slot(t, c), f_s.at[0, c], a_r.at[0, c], tp=sib)
        if kind == 1:
            return remote(a_slot(t, c), a_slot(t, c), f_s.at[1, c], a_r.at[1, c], tp=xn)
        return remote(a_slot(xn, c), a_slot(xn, c), f_s.at[2, c], a_r.at[2, c], tp=sib)

    def a_recv(rel, src, c):
        return remote(a_slot(src, c), a_slot(src, c), f_s.at[0, c], a_r.at[rel, c], tp=sib)

    def g_rows(u, r0, n, lane, width):
        return GU.at[u, pl.ds(1 + r0, n), pl.ds(1, HW), :, pl.ds(lane, width)]

    mine = al(LN * k, LN)
    theirs = al(LN * (1 - k), LN)

    def g2(c):
        return remote(g_rows(0, 7 * c, 7, 0, LN), g_rows(2, 7 * c, 7, mine, LN), g2_s.at[c], g2_r.at[c], tp=xn)

    def g3(p):
        return remote(g_rows(0, GP[p][0], GP[p][1], LN, LN), g_rows(3, GP[p][0], GP[p][1], mine, LN), g3_s.at[p], g3_r.at[p], tp=xn)

    def g2_rel(lane):
        return remote(g_rows(2, 0, HW, lane, LN), g_rows(2, 0, HW, lane, LN), rel_s.at[0], rel_r.at[0], tp=sib)

    def g3_rel(p, lane):
        return remote(g_rows(3, GP[p][0], GP[p][1], lane, LN), g_rows(3, GP[p][0], GP[p][1], lane, LN), rel_s.at[1 + p], rel_r.at[1 + p], tp=sib)

    def gdet(leg, p):
        r0, n = GP[p]
        own = g_rows(0, r0, n, LN, LN)
        a3 = g_rows(3, r0, n, mine, LN)
        a2 = g_rows(2, r0, n, mine, LN)
        src, dst, dev = ((own, a3, {"stage": 0}), (a3, a2, {"tp": xn}), (a2, a3, {"stage": 1}))[leg]
        return remote(src, dst, gd_s.at[leg, p - 2], gd_r.at[leg, p - 2], **dev)

    def det(leg, p):
        src, dst = ((W, WR), (WR, W), (W, WR))[leg]
        dev = ({"stage": 0}, {"dp": 1 - dp}, {"stage": 1})[leg]
        return remote(src.at[1, pl.ds(3 * p, 3)], dst.at[1, pl.ds(3 * p, 3)], d_s.at[leg, p], d_r.at[leg, p], **dev)

    def da_copy(s, n):
        return remote(DAO.at[pl.ds(2 * n, 2), :, pl.ds(2 * s, 2), :],
                      da_out.at[pl.ds(14 * k + 2 * n, 2), :, :, pl.ds(al(BLK * x, BLK), BLK)],
                      da_s.at[s, n], da_r.at[t, n], stage=0, tp=s)

    @pl.when(stage == 0)
    def _():
        a_cross().start()
        for c in range(CH):
            a_direct(c).start()
        a_cross().wait_recv()
        a_cross_fwd().start()
        W[0] = jnp.zeros((TAPS, LN, BLK), F32)

        def zrow(h, carry):
            DZ[h] = jnp.zeros((HW, NB, BLK), BF)
            return carry

        lax.fori_loop(0, HW, zrow, 0)
        outs = [pltpu.make_async_copy(W.at[0], dw_out.at[:, :, pl.ds(BLK * u, BLK)], out_s.at[u]) for u in range(4)]
        outs.append(pltpu.make_async_copy(DZ, z_out, out_s.at[4]))
        for o in outs:
            o.start()
        for o in outs:
            o.wait()
        for leg in range(2):
            for p in (2, 3):
                gdet(leg, p).wait_recv()
                gdet(leg + 1, p).start()
        for leg, p in ((0, 0), (0, 1), (1, 0), (0, 2), (1, 1), (1, 2)):
            det(leg, p).wait_recv()
            det(leg + 1, p).start()
        for c in range(CH):
            a_direct(c).wait_send()
        a_cross().wait_send()
        a_cross_fwd().wait_send()
        for p in range(3):
            det(1, p).wait_send()
            det(2, p).wait_send()
        for p in (2, 3):
            gdet(1, p).wait_send()
            gdet(2, p).wait_send()
        for src in range(4):
            for n in range(7):
                remote(DAO.at[pl.ds(2 * n, 2), :, pl.ds(0, 2), :],
                       da_out.at[pl.ds(14 * (src % 2) + 2 * n, 2), :, :, pl.ds(BLK * (src // 2), BLK)],
                       da_s.at[0, n], da_r.at[src, n], stage=0, tp=0).wait_recv()

    @pl.when(stage == 1)
    def _():
        k_copy(1, pz, t).start()
        k_copy(0, sib, t).start()
        for i, (u, lane, wd, src) in enumerate(kc_pieces(sib, t)):
            remote(w.at[:, :, pl.ds(al(src, LN), wd)], KCU.at[u, :, pl.ds(al(LN * k, LN), LN), pl.ds(lane, wd)],
                   kc_s.at[i], kc_r.at[i], tp=sib).start()
        loc = [pltpu.make_async_copy(w.at[:, :, pl.ds(al(src, LN), wd)], KCU.at[u, :, pl.ds(al(LN * k, LN), LN), pl.ds(lane, wd)], kc_l.at[i])
               for i, (u, lane, wd, src) in enumerate(kc_pieces(t, sib))]
        loc.append(pltpu.make_async_copy(w.at[:, :, pl.ds(al(BLK * t, BLK), BLK)], KO.at[:, pl.ds(al(LN * t, LN), LN), :], lsem.at[0]))
        loc.append(pltpu.make_async_copy(gz, DZ, lsem.at[1]))
        for o in loc:
            o.start()
        ZB[...] = jnp.zeros((7, HW, 2, CIN), BF)
        zcp = [pltpu.make_async_copy(ZB, da_out.at[pl.ds(7 * i, 7)], out_s.at[i]) for i in range(4)]
        for o in zcp:
            o.start()
        ACC[...] = jnp.zeros((14, RW, BLK), F32)

        for c in range(CH):
            a_recv(3, t, c).wait_recv()
            if c < 3:
                a_fwd(1, c).start()
            a_fwd(0, c).start()
            if c == 0:
                for o in loc:
                    o.wait()
                for o in zcp:
                    o.wait()
                for i, (u, lane, wd, src) in enumerate(kc_pieces(t, sib)):
                    remote(w.at[:, :, pl.ds(al(src, LN), wd)], KCU.at[u, :, pl.ds(al(LN * (1 - k), LN), LN), pl.ds(lane, wd)],
                           kc_s.at[i], kc_r.at[i], tp=sib).wait_recv()
            if c == 1:
                k_copy(1, t, pz).wait_recv()
                k_z(pz).start()

            def tr(tap, carry, c=c):
                KT[c, pl.ds(tap * BLK, BLK)] = KCU[c, tap].T
                return carry

            lax.fori_loop(0, TAPS, tr, 0)

        k_z(pz2).wait_recv()
        k_copy(0, t, sib).wait_recv()

        def row(h, carry):
            lhs = jnp.concatenate([A[h + i, j:j + HW].reshape(RW, CIN) for i in range(3) for j in range(3)], axis=1)
            pre = jnp.dot(lhs, KO[...].reshape(4608, BLK), preferred_element_type=F32)
            y = pre * sc[...] + sh[...]
            d = DZ[h].reshape(RW, BLK).astype(F32)
            g = jnp.where(y > 0, d * sc[...], 0.0).astype(BF)
            DZ[h] = jnp.maximum(y, 0.0).astype(BF).reshape(HW, NB, BLK)
            GU[0, h + 1, 1:29] = g.reshape(HW, NB, BLK)
            return carry

        z_cp = pltpu.make_async_copy(DZ, z_out, lsem.at[0])
        ac_cp = pltpu.make_async_copy(A.at[:, :, :, pl.ds(al(LN * t, LN), LN)], AC, lsem.at[1])
        g_sib = remote(GU.at[0], GU.at[1], gs_s.at[0], gs_r.at[0], tp=sib)

        for c in range(CH):
            a_recv(1, xn, c).wait_recv()
            a_fwd(2, c).start()
            a_recv(0, sib, c).wait_recv()
            a_recv(2, dg, c).wait_recv()
            if c == CH - 1:
                ac_cp.start()
            lax.fori_loop(7 * c, 7 * c + 7, row, 0)
            g2(c).start()
        for p in (2, 3):
            gdet(0, p).start()
        g_sib.start()
        z_cp.start()
        ac_cp.wait()

        zx = {u: remote(W.at[u], WR.at[u], zx_s.at[u], zx_r.at[u], dp=1 - dp) for u in (0, 2, 3)}

        def dw_unit(u):
            W[u] = jnp.zeros((TAPS, LN, BLK), F32)

            def step(n, carry):
                h = n * 7
                lhs = jnp.concatenate([AC[pl.ds(h + i, 7), j:j + HW].reshape(1568, LN) for i in range(3) for j in range(3)], axis=1)
                rhs = GU[u, pl.ds(h + 1, 7), 1:29].reshape(1568, BLK)
                p = lax.dot_general(lhs, rhs, (((0,), (0,)), ((), ())), preferred_element_type=F32)
                W[u] += p.reshape(TAPS, LN, BLK)
                return carry

            lax.fori_loop(0, 4, step, 0)
            if u == 1:
                for p in range(3):
                    det(0, p).start()
            else:
                zx[u].start()

        def da_rows(u, n):
            h = 14 * k + 2 * n
            lhs = jnp.concatenate([GU[u, pl.ds(h + 2 - i, 2), 2 - j:HP - j].reshape(448, BLK) for i in range(3) for j in range(3)], axis=1)
            return jnp.dot(lhs, KT[u], preferred_element_type=F32)

        def da_unit(u):
            def step(n, carry):
                ACC[pl.ds(2 * n, 2)] += da_rows(u, n).reshape(2, RW, BLK)
                return carry

            lax.fori_loop(0, 7, step, 0)

        dw_dst = ((BLK * t,), (BLK * sib,), (base, base + BLK), (base + LN, base + 384))

        def dw_out_cp(u):
            starts = dw_dst[u]
            wd = BLK // len(starts)
            return [pltpu.make_async_copy(WR.at[u, :, :, pl.ds(wd * i, wd)], dw_out.at[:, :, pl.ds(al(s, LN), wd)], kc_l.at[2 * (u // 2) + (u % 2) * (u // 2) + u % 2 + i])
                    for i, s in enumerate(starts)]

        def dw_final(u):
            if u == 1:
                for p in range(3):
                    det(2, p).wait_recv()
            else:
                zx[u].wait_recv()

            def add(q, carry):
                WR[u, q] += W[u, q]
                return carry

            lax.fori_loop(0, TAPS, add, 0)
            for o in dw_out_cp(u):
                o.start()

        dw_unit(0)
        g_sib.wait_recv()
        dw_unit(1)
        da_unit(0)
        da_unit(1)
        def last(n, carry):
            v = ACC[pl.ds(2 * n, 2)].reshape(448, BLK) + da_rows(3, n)
            DAO[pl.ds(2 * n, 2)] = v.astype(BF).reshape(2, HW, NB, BLK)
            for s in range(4):
                da_copy(s, n).start()
            return carry

        def g3_arrive(p):
            if p < 2:
                g3(p).wait_recv()
            else:
                gdet(2, p).wait_recv()
            g3_rel(p, mine).start()
            g3_rel(p, theirs).wait_recv()

        for c in range(CH):
            g2(c).wait_send()
        g3(0).start()
        for c in range(CH):
            g2(c).wait_recv()
        g2_rel(mine).start()
        g2_rel(theirs).wait_recv()
        dw_unit(2)
        g3(0).wait_send()
        g3(1).start()
        da_unit(2)
        g3_arrive(2)

        @pl.when(k == 1)
        def _():
            lax.fori_loop(4, 7, last, 0)

        g3_arrive(0)

        @pl.when(k == 0)
        def _():
            lax.fori_loop(0, 3, last, 0)

        dw_final(0)
        g3_arrive(3)
        g3_arrive(1)
        dw_unit(3)
        lax.fori_loop(3 - 3 * k, 7 - 3 * k, last, 0)
        dw_final(1)
        for u in range(2, 4):
            dw_final(u)

        z_cp.wait()
        for u in range(4):
            for o in dw_out_cp(u):
                o.wait()
            if u != 1:
                zx[u].wait_send()
        for p in range(3):
            det(0, p).wait_send()
        k_copy(1, pz, t).wait_send()
        k_z(pz).wait_send()
        k_copy(0, sib, t).wait_send()
        for i, (u, lane, wd, src) in enumerate(kc_pieces(sib, t)):
            remote(w.at[:, :, pl.ds(al(src, LN), wd)], KCU.at[u, :, pl.ds(al(LN * k, LN), LN), pl.ds(lane, wd)],
                   kc_s.at[i], kc_r.at[i], tp=sib).wait_send()
        for c in range(CH):
            for kind in range(3):
                if kind != 1 or c < 3:
                    a_fwd(kind, c).wait_send()
        g_sib.wait_send()
        g2_rel(mine).wait_send()
        g3(1).wait_send()
        for p in (2, 3):
            gdet(0, p).wait_send()
        for p in range(4):
            g3_rel(p, mine).wait_send()
        for s in range(4):
            for n in range(7):
                da_copy(s, n).wait_send()


def solution(mesh):
    V = pltpu.VMEM
    D = pltpu.SemaphoreType.DMA
    any_spec = pl.BlockSpec(memory_space=pl.ANY)
    vm_spec = pl.BlockSpec(memory_space=pltpu.VMEM)
    call = pl.pallas_call(
        kernel,
        out_shape=[jax.ShapeDtypeStruct((HW, HW, NB, BLK), BF), jax.ShapeDtypeStruct((HW, HW, 2, CIN), BF), jax.ShapeDtypeStruct((TAPS, LN, 1024), F32)],
        in_specs=[any_spec, any_spec, vm_spec, vm_spec, any_spec],
        out_specs=[any_spec] * 3,
        scratch_shapes=[
            V((HP, HP, NB, CIN), BF), V((HP, HP, NB, LN), BF), V((TAPS, CIN, BLK), BF), V((4, TAPS, BLK, BLK), BF), V((4, 2304, BLK), BF),
            V((HW, HW, NB, BLK), BF), V((4, HP, HP, NB, BLK), BF), V((4, TAPS, LN, BLK), F32), V((4, TAPS, LN, BLK), F32),
            V((14, RW, BLK), F32), V((14, HW, NB, BLK), BF), V((7, HW, 2, CIN), BF),
            D((2,)), D((3,)), D((3,)), D((6,)), D((6,)), D((6,)), D((6,)), D((1,)), D((4, 4)), D((3, 4)), D((1,)), D((1,)), D((4,)), D((4,)),
            D((2,)), D((2,)), D((3, 2)), D((3, 2)), D((5,)), D((5,)), D((4,)), D((4,)), D((3, 3)), D((3, 3)), D((4, 7)), D((4, 7)), D((5,)),
        ],
        compiler_params=pltpu.CompilerParams(collective_id=0, has_side_effects=True, vmem_limit_bytes=66000000),
        name="conv_block",
    )

    def body(act_loc, w_loc, scale_loc, shift_loc, grad_loc):
        z, da, dw = call(act_loc[0].transpose(1, 2, 0, 3), w_loc[0].reshape(TAPS, LN, 1024), scale_loc, shift_loc, grad_loc[0].transpose(1, 2, 0, 3))
        return z.transpose(2, 0, 1, 3)[None], da.transpose(2, 0, 1, 3)[None], dw.reshape(1, 3, 3, LN, 1024)

    act_spec = P("stage", ("dp", "tp"))
    w_spec = P("stage", None, None, "tp")
    vec_spec = P("stage", "tp")
    grad_spec = P("stage", "dp", None, None, "tp")
    return jax.shard_map(body, mesh=mesh, in_specs=(act_spec, w_spec, vec_spec, vec_spec, grad_spec), out_specs=(grad_spec, act_spec, w_spec), check_vma=False)
```

```python
import functools

import jax
import jax.numpy as jnp
from jax import lax
from jax.experimental import pallas as pl
from jax.experimental.pallas import tpu as pltpu
from jax.sharding import PartitionSpec as P

BF = jnp.bfloat16
F32 = jnp.float32
MESH = pl.DeviceIdType.MESH
CH = 7
CB = (0, 5, 9, 13, 17, 21, 25, 28)
GR = 4
CX = 5
GX = 4
DT = ((1, 0), (1, 1), (1, 2), (2, 2))
ZX = ((0, 0, 9), (2, 0, 6), (3, 0, 3), (3, 3, 3), (3, 6, 3))
HW = 28
HP = 30
NB = 8
RW = 224
TAPS = 9
LN = 128
BLK = 256
CIN = 512


def kernel(act, w, sc, sh, gz, z_out, da_out, dw_out, A, AC, KO, KCU, KT, DZ, GU, W, WR, ACC, DAO, ZB,
           lsem, ksem_s, ksem_r, kc_s, kc_r, kc_l, as_s, ax_s, ax_r, af_s, a_r, f_s, gs_s, gs_r, g_s, g_r, gd_s, gd_r, rel_s, rel_r,
           zx_s, zx_r, d_s, d_r, da_s, da_r, out_s):
    dp = lax.axis_index("dp")
    stage = lax.axis_index("stage")
    t = lax.axis_index("tp")
    x = t // 2
    k = t % 2
    sib = x * 2 + (1 - k)
    xn = (1 - x) * 2 + k
    dg = (1 - x) * 2 + (1 - k)
    pz = (1 - x) * 2 + (k + dp) % 2
    pz2 = (1 - x) * 2 + (k + 1 - dp) % 2
    base = (1 - x) * CIN

    def al(v, m):
        return pl.multiple_of(v, m)

    def remote(src, dst, ssem, rsem, **dev):
        return pltpu.make_async_remote_copy(src_ref=src, dst_ref=dst, send_sem=ssem, recv_sem=rsem, device_id=dev, device_id_type=MESH)

    A[0] = jnp.zeros((HP, NB, CIN), BF)
    A[29] = jnp.zeros((HP, NB, CIN), BF)
    A[:, 0] = jnp.zeros((HP, NB, CIN), BF)
    A[:, 29] = jnp.zeros((HP, NB, CIN), BF)

    def zero_halo(u, carry):
        GU[u, 0] = jnp.zeros((HP, NB, BLK), BF)
        GU[u, 29] = jnp.zeros((HP, NB, BLK), BF)
        GU[u, :, 0] = jnp.zeros((HP, NB, BLK), BF)
        GU[u, :, 29] = jnp.zeros((HP, NB, BLK), BF)
        return carry

    lax.fori_loop(0, 4, zero_halo, 0)

    barrier = pltpu.get_barrier_semaphore()
    for ds in range(2):
        for dt in range(4):
            if ds or dt:
                pl.semaphore_signal(barrier, inc=1, device_id={"stage": (stage + ds) % 2, "tp": (t + dt) % 4}, device_id_type=MESH)
    pl.semaphore_signal(barrier, inc=1, device_id={"dp": 1 - dp}, device_id_type=MESH)
    pl.semaphore_wait(barrier, NB)

    def k_slot(src_tp):
        return KO.at[:, pl.ds(al(LN * src_tp, LN), LN), :]

    def k_copy(rel, peer, src_tp):
        return remote(w.at[:, :, pl.ds(al(BLK * peer, BLK), BLK)], k_slot(src_tp), ksem_s.at[rel], ksem_r.at[rel], tp=peer)

    def k_z(src_tp):
        return remote(k_slot(src_tp), k_slot(src_tp), ksem_s.at[2], ksem_r.at[2], dp=1 - dp)

    def kc_pieces(own, other):
        return ((0, 0, BLK, BLK * own), (1, 0, BLK, BLK * other), (2, 0, LN, base), (2, LN, LN, base + BLK),
                (3, 0, LN, base + LN), (3, LN, LN, base + 384))

    def a_slot(src, c):
        return A.at[pl.ds(1 + CB[c], CB[c + 1] - CB[c]), pl.ds(1, HW), pl.ds(2 * src, 2), :]

    def a_direct(c):
        return remote(act.at[pl.ds(CB[c], CB[c + 1] - CB[c])], a_slot(t, c), as_s.at[c], a_r.at[3, c], stage=1)

    def a_cross(c):
        return remote(act.at[pl.ds(CB[c], CB[c + 1] - CB[c])], a_slot(t, c), ax_s.at[c - CX], ax_r.at[c - CX], tp=xn)

    def a_cross_fwd(c):
        return remote(a_slot(xn, c), a_slot(xn, c), af_s.at[c - CX], a_r.at[1, c], stage=1)

    def a_fwd(kind, c):
        if kind == 0:
            return remote(a_slot(t, c), a_slot(t, c), f_s.at[0, c], a_r.at[0, c], tp=sib)
        if kind == 1:
            return remote(a_slot(t, c), a_slot(t, c), f_s.at[1, c], a_r.at[1, c], tp=xn)
        return remote(a_slot(xn, c), a_slot(xn, c), f_s.at[2, c], a_r.at[2, c], tp=sib)

    def a_recv(rel, src, c):
        return remote(a_slot(src, c), a_slot(src, c), f_s.at[0, c], a_r.at[rel, c], tp=sib)

    def g_rows(u, r0, n, lane, width):
        return GU.at[u, pl.ds(1 + r0, n), pl.ds(1, HW), :, pl.ds(lane, width)]

    mine = al(LN * k, LN)
    theirs = al(LN * (1 - k), LN)

    def g_x(u, c):
        return remote(g_rows(0, GR * c, GR, LN * (u - 2), LN), g_rows(u, GR * c, GR, mine, LN), g_s.at[u - 2, c], g_r.at[u - 2, c], tp=xn)

    def g_rel(u, c, lane):
        return remote(g_rows(u, GR * c, GR, lane, LN), g_rows(u, GR * c, GR, lane, LN), rel_s.at[u - 2, c], rel_r.at[u - 2, c], tp=sib)

    def gdet(leg, c):
        own = g_rows(0, GR * c, GR, LN, LN)
        a3 = g_rows(3, GR * c, GR, mine, LN)
        a2 = g_rows(2, GR * c, GR, mine, LN)
        src, dst, dev = ((own, a3, {"stage": 0}), (a3, a2, {"tp": xn}), (a2, a3, {"stage": 1}))[leg]
        return remote(src, dst, gd_s.at[leg, c], gd_r.at[leg, c], **dev)

    def det(leg, q):
        src, dst = ((W, WR), (WR, W), (W, WR))[leg]
        dev = ({"stage": 0}, {"dp": 1 - dp}, {"stage": 1})[leg]
        u, p = DT[q]
        return remote(src.at[u, pl.ds(3 * p, 3)], dst.at[u, pl.ds(3 * p, 3)], d_s.at[leg, q], d_r.at[leg, q], **dev)

    def zx(q):
        u, p, n = ZX[q]
        return remote(W.at[u, pl.ds(p, n)], WR.at[u, pl.ds(p, n)], zx_s.at[q], zx_r.at[q], dp=1 - dp)

    def da_copy(s, n):
        return remote(DAO.at[pl.ds(2 * n, 2), :, pl.ds(2 * s, 2), :],
                      da_out.at[pl.ds(14 * k + 2 * n, 2), :, :, pl.ds(al(BLK * x, BLK), BLK)],
                      da_s.at[s, n], da_r.at[t, n], stage=0, tp=s)

    @pl.when(stage == 0)
    def _():
        for c in range(CX, CH):
            a_cross(c).start()
        for c in range(CH):
            a_direct(c).start()
        for c in range(CX, CH):
            a_cross(c).wait_recv()
            a_cross_fwd(c).start()
        W[0] = jnp.zeros((TAPS, LN, BLK), F32)

        def zrow(h, carry):
            DZ[h] = jnp.zeros((HW, NB, BLK), BF)
            return carry

        lax.fori_loop(0, HW, zrow, 0)
        outs = [pltpu.make_async_copy(W.at[0], dw_out.at[:, :, pl.ds(BLK * u, BLK)], out_s.at[u]) for u in range(4)]
        outs.append(pltpu.make_async_copy(DZ, z_out, out_s.at[4]))
        for o in outs:
            o.start()
        for o in outs:
            o.wait()
        for c in range(GX):
            gdet(0, c).wait_recv()
            gdet(1, c).start()
        for c in range(CH):
            a_direct(c).wait_send()
        for c in range(CX, CH):
            a_cross(c).wait_send()
            a_cross_fwd(c).wait_send()
        for c in range(GX):
            gdet(1, c).wait_recv()
            gdet(2, c).start()
        for leg, q in ((0, 0), (0, 1), (1, 0), (0, 2), (1, 1), (1, 2), (0, 3), (1, 3)):
            det(leg, q).wait_recv()
            det(leg + 1, q).start()
        for q in range(4):
            det(1, q).wait_send()
            det(2, q).wait_send()
        for c in range(GX):
            gdet(1, c).wait_send()
            gdet(2, c).wait_send()
        for src in range(4):
            for n in range(7):
                remote(DAO.at[pl.ds(2 * n, 2), :, pl.ds(0, 2), :],
                       da_out.at[pl.ds(14 * (src % 2) + 2 * n, 2), :, :, pl.ds(BLK * (src // 2), BLK)],
                       da_s.at[0, n], da_r.at[src, n], stage=0, tp=0).wait_recv()

    @pl.when(stage == 1)
    def _():
        k_copy(1, pz, t).start()
        k_copy(0, sib, t).start()
        for i, (u, lane, wd, src) in enumerate(kc_pieces(sib, t)):
            remote(w.at[:, :, pl.ds(al(src, LN), wd)], KCU.at[u, :, pl.ds(al(LN * k, LN), LN), pl.ds(lane, wd)],
                   kc_s.at[i], kc_r.at[i], tp=sib).start()
        loc = [pltpu.make_async_copy(w.at[:, :, pl.ds(al(src, LN), wd)], KCU.at[u, :, pl.ds(al(LN * k, LN), LN), pl.ds(lane, wd)], kc_l.at[i])
               for i, (u, lane, wd, src) in enumerate(kc_pieces(t, sib))]
        loc.append(pltpu.make_async_copy(w.at[:, :, pl.ds(al(BLK * t, BLK), BLK)], KO.at[:, pl.ds(al(LN * t, LN), LN), :], lsem.at[0]))
        loc.append(pltpu.make_async_copy(gz, DZ, lsem.at[1]))
        for o in loc:
            o.start()
        ZB[...] = jnp.zeros((7, HW, 2, CIN), BF)
        zcp = [pltpu.make_async_copy(ZB, da_out.at[pl.ds(7 * i, 7)], out_s.at[i]) for i in range(4)]
        for o in zcp:
            o.start()
        ACC[...] = jnp.zeros((14, RW, BLK), F32)
        W[...] = jnp.zeros((4, TAPS, LN, BLK), F32)
        AC[0] = jnp.zeros((HP, NB, LN), BF)
        AC[29] = jnp.zeros((HP, NB, LN), BF)

        def forward_images(c):
            a_recv(3, t, c).wait_recv()
            if c < CX:
                a_fwd(1, c).start()
            a_fwd(0, c).start()

        def transpose(u):
            def tr(tap, carry):
                KT[u, pl.ds(tap * BLK, BLK)] = KCU[u, tap].T
                return carry

            lax.fori_loop(0, TAPS, tr, 0)

        forward_images(0)
        for o in loc:
            o.wait()
        for o in zcp:
            o.wait()
        for i, (u, lane, wd, src) in enumerate(kc_pieces(t, sib)):
            remote(w.at[:, :, pl.ds(al(src, LN), wd)], KCU.at[u, :, pl.ds(theirs, LN), pl.ds(lane, wd)],
                   kc_s.at[i], kc_r.at[i], tp=sib).wait_recv()
        transpose(0)
        transpose(1)
        forward_images(1)
        k_copy(1, t, pz).wait_recv()
        k_z(pz).start()
        transpose(2)
        forward_images(2)
        transpose(3)

        def row(h, carry):
            lhs = jnp.concatenate([A[h + i, j:j + HW].reshape(RW, CIN) for i in range(3) for j in range(3)], axis=1)
            pre = jnp.dot(lhs, KO[...].reshape(4608, BLK), preferred_element_type=F32)
            y = pre * sc[...] + sh[...]
            d = DZ[h].reshape(RW, BLK).astype(F32)
            g = jnp.where(y > 0, d * sc[...], 0.0).astype(BF)
            DZ[h] = jnp.maximum(y, 0.0).astype(BF).reshape(HW, NB, BLK)
            GU[0, h + 1, 1:29] = g.reshape(HW, NB, BLK)
            return carry

        z_cp = pltpu.make_async_copy(DZ, z_out, lsem.at[0])
        g_sib = remote(GU.at[0], GU.at[1], gs_s.at[0], gs_r.at[0], tp=sib)

        for c in range(CH):
            if c + 3 < CH:
                forward_images(c + 3)
            if c == 0:
                k_z(pz2).wait_recv()
                k_copy(0, t, sib).wait_recv()
            a_recv(1, xn, c).wait_recv()
            a_fwd(2, c).start()
            a_recv(0, sib, c).wait_recv()
            a_recv(2, dg, c).wait_recv()
            new = pl.ds(1 + CB[c], CB[c + 1] - CB[c])
            AC[new] = A[new, :, :, pl.ds(al(LN * t, LN), LN)]
            lax.fori_loop(GR * c, GR * c + GR, row, 0)
            if c < GX:
                gdet(0, c).start()
            if c == 1:
                g_x(2, 0).start()
            if c > 0:
                g_x(2, c).start()
        g_sib.start()
        z_cp.start()

        def dw_step(u, n):
            h = n * 7
            lhs = jnp.concatenate([AC[pl.ds(h + i, 7), j:j + HW].reshape(1568, LN) for i in range(3) for j in range(3)], axis=1)
            rhs = GU[u, pl.ds(h + 1, 7), 1:29].reshape(1568, BLK)
            p = lax.dot_general(lhs, rhs, (((0,), (0,)), ((), ())), preferred_element_type=F32)
            W[u] += p.reshape(TAPS, LN, BLK)

        def dw_steps(u, lo, hi):
            def step(n, carry):
                dw_step(u, n)
                return carry

            lax.fori_loop(lo, hi, step, 0)

        def dw_send(u):
            for q, d in enumerate(DT):
                if d[0] == u:
                    det(0, q).start()
            for q, d in enumerate(ZX):
                if d[0] == u:
                    zx(q).start()

        def da_rows(u, n):
            h = 14 * k + 2 * n
            lhs = jnp.concatenate([GU[u, pl.ds(h + 2 - i, 2), 2 - j:HP - j].reshape(448, BLK) for i in range(3) for j in range(3)], axis=1)
            return jnp.dot(lhs, KT[u], preferred_element_type=F32)

        def da_unit(u):
            def step(n, carry):
                ACC[pl.ds(2 * n, 2)] += da_rows(u, n).reshape(2, RW, BLK)
                return carry

            lax.fori_loop(0, 7, step, 0)

        dw_dst = ((BLK * t,), (BLK * sib,), (base, base + BLK), (base + LN, base + 384))

        def dw_out_cp(u):
            starts = dw_dst[u]
            wd = BLK // len(starts)
            return [pltpu.make_async_copy(WR.at[u, :, :, pl.ds(wd * i, wd)], dw_out.at[:, :, pl.ds(al(s, LN), wd)], kc_l.at[2 * (u // 2) + (u % 2) * (u // 2) + u % 2 + i])
                    for i, s in enumerate(starts)]

        def dw_final(u):
            for q, d in enumerate(DT):
                if d[0] == u:
                    det(2, q).wait_recv()
            for q, d in enumerate(ZX):
                if d[0] == u:
                    zx(q).wait_recv()

            def add(q, carry):
                WR[u, q] += W[u, q]
                return carry

            lax.fori_loop(0, TAPS, add, 0)
            for o in dw_out_cp(u):
                o.start()

        dw_steps(0, 0, 4)
        dw_send(0)
        g_sib.wait_recv()
        dw_steps(1, 0, 4)
        dw_send(1)
        da_unit(0)
        da_unit(1)

        def last(n, carry):
            v = ACC[pl.ds(2 * n, 2)].reshape(448, BLK) + da_rows(3, n)
            DAO[pl.ds(2 * n, 2)] = v.astype(BF).reshape(2, HW, NB, BLK)
            for s in range(4):
                da_copy(s, n).start()
            return carry

        def arrive(u, lo, hi):
            for c in range(lo, hi):
                if u == 3 and c < GX:
                    gdet(2, c).wait_recv()
                else:
                    g_x(u, c).wait_recv()
                g_rel(u, c, mine).start()
            for c in range(lo, hi):
                g_rel(u, c, theirs).wait_recv()

        arrive(2, 0, 4)
        dw_steps(2, 0, 2)
        arrive(2, 4, 6)
        dw_steps(2, 2, 3)
        for c in range(CH):
            g_x(2, c).wait_send()
        for c in range(GX, CH):
            g_x(3, c).start()
        arrive(2, 6, 7)
        dw_steps(2, 3, 4)
        dw_send(2)
        da_unit(2)
        arrive(3, 0, 4)

        @pl.when(k == 0)
        def _():
            lax.fori_loop(0, 7, last, 0)

        dw_steps(3, 0, 2)
        dw_final(0)
        arrive(3, 4, 6)
        dw_steps(3, 2, 3)

        @pl.when(k == 1)
        def _():
            lax.fori_loop(0, 4, last, 0)

        arrive(3, 6, 7)
        dw_steps(3, 3, 4)
        dw_send(3)

        @pl.when(k == 1)
        def _():
            lax.fori_loop(4, 7, last, 0)

        dw_final(1)
        for u in range(2, 4):
            dw_final(u)

        z_cp.wait()
        for u in range(4):
            for o in dw_out_cp(u):
                o.wait()
        for q in range(4):
            det(0, q).wait_send()
        for q in range(5):
            zx(q).wait_send()
        k_copy(1, pz, t).wait_send()
        k_z(pz).wait_send()
        k_copy(0, sib, t).wait_send()
        for i, (u, lane, wd, src) in enumerate(kc_pieces(sib, t)):
            remote(w.at[:, :, pl.ds(al(src, LN), wd)], KCU.at[u, :, pl.ds(al(LN * k, LN), LN), pl.ds(lane, wd)],
                   kc_s.at[i], kc_r.at[i], tp=sib).wait_send()
        for c in range(CH):
            for kind in range(3):
                if kind != 1 or c < CX:
                    a_fwd(kind, c).wait_send()
            g_rel(2, c, mine).wait_send()
            g_rel(3, c, mine).wait_send()
            if c < GX:
                gdet(0, c).wait_send()
            else:
                g_x(3, c).wait_send()
        g_sib.wait_send()
        for s in range(4):
            for n in range(7):
                da_copy(s, n).wait_send()


def solution(mesh):
    V = pltpu.VMEM
    D = pltpu.SemaphoreType.DMA
    any_spec = pl.BlockSpec(memory_space=pl.ANY)
    vm_spec = pl.BlockSpec(memory_space=pltpu.VMEM)
    call = pl.pallas_call(
        kernel,
        out_shape=[jax.ShapeDtypeStruct((HW, HW, NB, BLK), BF), jax.ShapeDtypeStruct((HW, HW, 2, CIN), BF), jax.ShapeDtypeStruct((TAPS, LN, 1024), F32)],
        in_specs=[any_spec, any_spec, vm_spec, vm_spec, any_spec],
        out_specs=[any_spec] * 3,
        scratch_shapes=[
            V((HP, HP, NB, CIN), BF), V((HP, HP, NB, LN), BF), V((TAPS, CIN, BLK), BF), V((4, TAPS, BLK, BLK), BF), V((4, 2304, BLK), BF),
            V((HW, HW, NB, BLK), BF), V((4, HP, HP, NB, BLK), BF), V((4, TAPS, LN, BLK), F32), V((4, TAPS, LN, BLK), F32),
            V((14, RW, BLK), F32), V((14, HW, NB, BLK), BF), V((7, HW, 2, CIN), BF),
            D((2,)), D((3,)), D((3,)), D((6,)), D((6,)), D((6,)), D((CH,)), D((2,)), D((2,)), D((2,)), D((4, CH)), D((3, CH)), D((1,)), D((1,)),
            D((2, CH)), D((2, CH)), D((3, GX)), D((3, GX)), D((2, CH)), D((2, CH)), D((5,)), D((5,)), D((3, 4)), D((3, 4)), D((4, 7)), D((4, 7)), D((5,)),
        ],
        compiler_params=pltpu.CompilerParams(collective_id=0, has_side_effects=True, vmem_limit_bytes=66000000),
        name="conv_block",
    )

    def body(act_loc, w_loc, scale_loc, shift_loc, grad_loc):
        z, da, dw = call(act_loc[0].transpose(1, 2, 0, 3), w_loc[0].reshape(TAPS, LN, 1024), scale_loc, shift_loc, grad_loc[0].transpose(1, 2, 0, 3))
        return z.transpose(2, 0, 1, 3)[None], da.transpose(2, 0, 1, 3)[None], dw.reshape(1, 3, 3, LN, 1024)

    act_spec = P("stage", ("dp", "tp"))
    w_spec = P("stage", None, None, "tp")
    vec_spec = P("stage", "tp")
    grad_spec = P("stage", "dp", None, None, "tp")
    return jax.shard_map(body, mesh=mesh, in_specs=(act_spec, w_spec, vec_spec, vec_spec, grad_spec), out_specs=(grad_spec, act_spec, w_spec), check_vma=False)
```

```python
import functools

import jax
import jax.numpy as jnp
from jax import lax
from jax.experimental import pallas as pl
from jax.experimental.pallas import tpu as pltpu
from jax.sharding import PartitionSpec as P

BF = jnp.bfloat16
F32 = jnp.float32
MESH = pl.DeviceIdType.MESH
CH = 7
CB = (0, 5, 9, 13, 17, 21, 25, 28)
GR = 4
CX = 5
GX = 4
DT = ((1, 0), (1, 1), (1, 2), (2, 2))
ZX = ((0, 0, 9), (2, 0, 6), (3, 0, 3), (3, 3, 3), (3, 6, 3))
HW = 28
HP = 30
NB = 8
RW = 224
TAPS = 9
LN = 128
BLK = 256
CIN = 512


def kernel(act, w, sc, sh, gz, z_out, da_out, dw_out, A, AC, KO, KCU, KT, DZ, GU, W, WR, ACC, DAO, ZB, L, DAL,
           lsem, ksem_s, ksem_r, kc_s, kc_r, kc_l, as_s, ax_s, ax_r, af_s, a_r, f_s, gs_s, gs_r, g_s, g_r, gd_s, gd_r, rel_s, rel_r,
           zx_s, zx_r, d_s, d_r, da_s, da_r, out_s):
    dp = lax.axis_index("dp")
    stage = lax.axis_index("stage")
    t = lax.axis_index("tp")
    x = t // 2
    k = t % 2
    sib = x * 2 + (1 - k)
    xn = (1 - x) * 2 + k
    dg = (1 - x) * 2 + (1 - k)
    pz = (1 - x) * 2 + (k + dp) % 2
    pz2 = (1 - x) * 2 + (k + 1 - dp) % 2
    base = (1 - x) * CIN

    def al(v, m):
        return pl.multiple_of(v, m)

    def remote(src, dst, ssem, rsem, **dev):
        return pltpu.make_async_remote_copy(src_ref=src, dst_ref=dst, send_sem=ssem, recv_sem=rsem, device_id=dev, device_id_type=MESH)

    A[0] = jnp.zeros((HP, NB, CIN), BF)
    A[29] = jnp.zeros((HP, NB, CIN), BF)
    A[:, 0] = jnp.zeros((HP, NB, CIN), BF)
    A[:, 29] = jnp.zeros((HP, NB, CIN), BF)

    def zero_halo(u, carry):
        GU[u, 0] = jnp.zeros((HP, NB, BLK), BF)
        GU[u, 29] = jnp.zeros((HP, NB, BLK), BF)
        GU[u, :, 0] = jnp.zeros((HP, NB, BLK), BF)
        GU[u, :, 29] = jnp.zeros((HP, NB, BLK), BF)
        return carry

    lax.fori_loop(0, 4, zero_halo, 0)

    barrier = pltpu.get_barrier_semaphore()
    for ds in range(2):
        for dt in range(4):
            if ds or dt:
                pl.semaphore_signal(barrier, inc=1, device_id={"stage": (stage + ds) % 2, "tp": (t + dt) % 4}, device_id_type=MESH)
    pl.semaphore_signal(barrier, inc=1, device_id={"dp": 1 - dp}, device_id_type=MESH)
    pl.semaphore_wait(barrier, NB)

    def k_slot(src_tp):
        return KO.at[:, pl.ds(al(LN * src_tp, LN), LN), :]

    def k_copy(rel, peer, src_tp):
        return remote(w.at[:, :, pl.ds(al(BLK * peer, BLK), BLK)], k_slot(src_tp), ksem_s.at[rel], ksem_r.at[rel], tp=peer)

    def k_z(src_tp):
        return remote(k_slot(src_tp), k_slot(src_tp), ksem_s.at[2], ksem_r.at[2], dp=1 - dp)

    def kc_pieces(own, other):
        return ((0, 0, BLK, BLK * own), (1, 0, BLK, BLK * other), (2, 0, LN, base), (2, LN, LN, base + BLK),
                (3, 0, LN, base + LN), (3, LN, LN, base + 384))

    def a_slot(src, c):
        return L.at[src, pl.ds(CB[c], CB[c + 1] - CB[c])]

    def a_direct(c):
        return remote(act.at[pl.ds(CB[c], CB[c + 1] - CB[c])], a_slot(t, c), as_s.at[c], a_r.at[3, c], stage=1)

    def a_cross(c):
        return remote(act.at[pl.ds(CB[c], CB[c + 1] - CB[c])], a_slot(t, c), ax_s.at[c - CX], ax_r.at[c - CX], tp=xn)

    def a_cross_fwd(c):
        return remote(a_slot(xn, c), a_slot(xn, c), af_s.at[c - CX], a_r.at[1, c], stage=1)

    def a_fwd(kind, c):
        if kind == 0:
            return remote(a_slot(t, c), a_slot(t, c), f_s.at[0, c], a_r.at[0, c], tp=sib)
        if kind == 1:
            return remote(a_slot(t, c), a_slot(t, c), f_s.at[1, c], a_r.at[1, c], tp=xn)
        return remote(a_slot(xn, c), a_slot(xn, c), f_s.at[2, c], a_r.at[2, c], tp=sib)

    def a_recv(rel, src, c):
        return remote(a_slot(src, c), a_slot(src, c), f_s.at[0, c], a_r.at[rel, c], tp=sib)

    def g_rows(u, r0, n, lane, width):
        return GU.at[u, pl.ds(1 + r0, n), pl.ds(1, HW), :, pl.ds(lane, width)]

    mine = al(LN * k, LN)
    theirs = al(LN * (1 - k), LN)

    def g_x(u, c):
        return remote(g_rows(0, GR * c, GR, LN * (u - 2), LN), g_rows(u, GR * c, GR, mine, LN), g_s.at[u - 2, c], g_r.at[u - 2, c], tp=xn)

    def g_rel(u, c, lane):
        return remote(g_rows(u, GR * c, GR, lane, LN), g_rows(u, GR * c, GR, lane, LN), rel_s.at[u - 2, c], rel_r.at[u - 2, c], tp=sib)

    def gdet(leg, c):
        own = g_rows(0, GR * c, GR, LN, LN)
        a3 = g_rows(3, GR * c, GR, mine, LN)
        a2 = g_rows(2, GR * c, GR, mine, LN)
        src, dst, dev = ((own, a3, {"stage": 0}), (a3, a2, {"tp": xn}), (a2, a3, {"stage": 1}))[leg]
        return remote(src, dst, gd_s.at[leg, c], gd_r.at[leg, c], **dev)

    def det(leg, q):
        src, dst = ((W, WR), (WR, W), (W, WR))[leg]
        dev = ({"stage": 0}, {"dp": 1 - dp}, {"stage": 1})[leg]
        u, p = DT[q]
        return remote(src.at[u, pl.ds(3 * p, 3)], dst.at[u, pl.ds(3 * p, 3)], d_s.at[leg, q], d_r.at[leg, q], **dev)

    def zx(q):
        u, p, n = ZX[q]
        return remote(W.at[u, pl.ds(p, n)], WR.at[u, pl.ds(p, n)], zx_s.at[q], zx_r.at[q], dp=1 - dp)

    def da_copy(s, n):
        return remote(DAO.at[s, pl.ds(2 * n, 2)], DAL.at[x, pl.ds(14 * k + 2 * n, 2)], da_s.at[s, n], da_r.at[t, n], stage=0, tp=s)

    @pl.when(stage == 0)
    def _():
        for c in range(CX, CH):
            a_cross(c).start()
        for c in range(CH):
            a_direct(c).start()
        for c in range(CX, CH):
            a_cross(c).wait_recv()
            a_cross_fwd(c).start()
        W[0] = jnp.zeros((TAPS, LN, BLK), F32)

        def zrow(h, carry):
            DZ[h] = jnp.zeros((HW, NB, BLK), BF)
            return carry

        lax.fori_loop(0, HW, zrow, 0)
        outs = [pltpu.make_async_copy(W.at[0], dw_out.at[:, :, pl.ds(BLK * u, BLK)], out_s.at[u]) for u in range(4)]
        outs.append(pltpu.make_async_copy(DZ, z_out, out_s.at[4]))
        for o in outs:
            o.start()
        for o in outs:
            o.wait()
        for c in range(GX):
            gdet(0, c).wait_recv()
            gdet(1, c).start()
        for c in range(CH):
            a_direct(c).wait_send()
        for c in range(CX, CH):
            a_cross(c).wait_send()
            a_cross_fwd(c).wait_send()
        for c in range(GX):
            gdet(1, c).wait_recv()
            gdet(2, c).start()
        for leg, q in ((0, 0), (0, 1), (1, 0), (0, 2), (1, 1), (1, 2), (0, 3), (1, 3)):
            det(leg, q).wait_recv()
            det(leg + 1, q).start()
        for q in range(4):
            det(1, q).wait_send()
            det(2, q).wait_send()
        for c in range(GX):
            gdet(1, c).wait_send()
            gdet(2, c).wait_send()
        outs = []
        for src in (0, 2, 1, 3):
            for n in range(7):
                rows = pl.ds(14 * (src % 2) + 2 * n, 2)
                remote(DAO.at[0, pl.ds(2 * n, 2)], DAL.at[src // 2, rows], da_s.at[0, n], da_r.at[src, n], stage=0, tp=0).wait_recv()
                o = pltpu.make_async_copy(DAL.at[src // 2, rows], da_out.at[rows, :, :, pl.ds(BLK * (src // 2), BLK)], da_s.at[src, n])
                o.start()
                outs.append(o)
        for o in outs:
            o.wait()

    @pl.when(stage == 1)
    def _():
        k_copy(1, pz, t).start()
        k_copy(0, sib, t).start()
        for i, (u, lane, wd, src) in enumerate(kc_pieces(sib, t)):
            remote(w.at[:, :, pl.ds(al(src, LN), wd)], KCU.at[u, :, pl.ds(al(LN * k, LN), LN), pl.ds(lane, wd)],
                   kc_s.at[i], kc_r.at[i], tp=sib).start()
        loc = [pltpu.make_async_copy(w.at[:, :, pl.ds(al(src, LN), wd)], KCU.at[u, :, pl.ds(al(LN * k, LN), LN), pl.ds(lane, wd)], kc_l.at[i])
               for i, (u, lane, wd, src) in enumerate(kc_pieces(t, sib))]
        loc.append(pltpu.make_async_copy(w.at[:, :, pl.ds(al(BLK * t, BLK), BLK)], KO.at[:, pl.ds(al(LN * t, LN), LN), :], lsem.at[0]))
        loc.append(pltpu.make_async_copy(gz, DZ, lsem.at[1]))
        for o in loc:
            o.start()
        ZB[...] = jnp.zeros((7, HW, 2, CIN), BF)
        zcp = [pltpu.make_async_copy(ZB, da_out.at[pl.ds(7 * i, 7)], out_s.at[i]) for i in range(4)]
        for o in zcp:
            o.start()
        ACC[...] = jnp.zeros((14, RW, BLK), F32)
        W[...] = jnp.zeros((4, TAPS, LN, BLK), F32)
        AC[0] = jnp.zeros((HP, NB, LN), BF)
        AC[29] = jnp.zeros((HP, NB, LN), BF)

        def forward_images(c):
            a_recv(3, t, c).wait_recv()
            if c < CX:
                a_fwd(1, c).start()
            a_fwd(0, c).start()

        def transpose(u):
            def tr(tap, carry):
                KT[u, pl.ds(tap * BLK, BLK)] = KCU[u, tap].T
                return carry

            lax.fori_loop(0, TAPS, tr, 0)

        forward_images(0)
        for o in loc:
            o.wait()
        for o in zcp:
            o.wait()
        for i, (u, lane, wd, src) in enumerate(kc_pieces(t, sib)):
            remote(w.at[:, :, pl.ds(al(src, LN), wd)], KCU.at[u, :, pl.ds(theirs, LN), pl.ds(lane, wd)],
                   kc_s.at[i], kc_r.at[i], tp=sib).wait_recv()
        transpose(0)
        transpose(1)
        forward_images(1)
        k_copy(1, t, pz).wait_recv()
        k_z(pz).start()
        transpose(2)
        forward_images(2)
        transpose(3)

        def merge(h, carry):
            A[h + 1, 1:29] = jnp.concatenate([L[s, h] for s in range(4)], axis=1)
            return carry

        def row(h, carry):
            lhs = jnp.concatenate([A[h + i, j:j + HW].reshape(RW, CIN) for i in range(3) for j in range(3)], axis=1)
            pre = jnp.dot(lhs, KO[...].reshape(4608, BLK), preferred_element_type=F32)
            y = pre * sc[...] + sh[...]
            d = DZ[h].reshape(RW, BLK).astype(F32)
            g = jnp.where(y > 0, d * sc[...], 0.0).astype(BF)
            DZ[h] = jnp.maximum(y, 0.0).astype(BF).reshape(HW, NB, BLK)
            GU[0, h + 1, 1:29] = g.reshape(HW, NB, BLK)
            return carry

        z_cp = pltpu.make_async_copy(DZ, z_out, lsem.at[0])
        g_sib = remote(GU.at[0], GU.at[1], gs_s.at[0], gs_r.at[0], tp=sib)

        for c in range(CH):
            if c + 3 < CH:
                forward_images(c + 3)
            if c == 0:
                k_z(pz2).wait_recv()
                k_copy(0, t, sib).wait_recv()
            a_recv(1, xn, c).wait_recv()
            a_fwd(2, c).start()
            a_recv(0, sib, c).wait_recv()
            a_recv(2, dg, c).wait_recv()
            lax.fori_loop(CB[c], CB[c + 1], merge, 0)
            new = pl.ds(1 + CB[c], CB[c + 1] - CB[c])
            AC[new] = A[new, :, :, pl.ds(al(LN * t, LN), LN)]
            lax.fori_loop(GR * c, GR * c + GR, row, 0)
            if c < GX:
                gdet(0, c).start()
            if c == 1:
                g_x(2, 0).start()
            if c > 0:
                g_x(2, c).start()
        g_sib.start()
        z_cp.start()

        def dw_step(u, n):
            h = n * 7
            lhs = jnp.concatenate([AC[pl.ds(h + i, 7), j:j + HW].reshape(1568, LN) for i in range(3) for j in range(3)], axis=1)
            rhs = GU[u, pl.ds(h + 1, 7), 1:29].reshape(1568, BLK)
            p = lax.dot_general(lhs, rhs, (((0,), (0,)), ((), ())), preferred_element_type=F32)
            W[u] += p.reshape(TAPS, LN, BLK)

        def dw_steps(u, lo, hi):
            def step(n, carry):
                dw_step(u, n)
                return carry

            lax.fori_loop(lo, hi, step, 0)

        def dw_send(u):
            for q, d in enumerate(DT):
                if d[0] == u:
                    det(0, q).start()
            for q, d in enumerate(ZX):
                if d[0] == u:
                    zx(q).start()

        def da_rows(u, n):
            h = 14 * k + 2 * n
            lhs = jnp.concatenate([GU[u, pl.ds(h + 2 - i, 2), 2 - j:HP - j].reshape(448, BLK) for i in range(3) for j in range(3)], axis=1)
            return jnp.dot(lhs, KT[u], preferred_element_type=F32)

        def da_unit(u):
            def step(n, carry):
                ACC[pl.ds(2 * n, 2)] += da_rows(u, n).reshape(2, RW, BLK)
                return carry

            lax.fori_loop(0, 7, step, 0)

        dw_dst = ((BLK * t,), (BLK * sib,), (base, base + BLK), (base + LN, base + 384))

        def dw_out_cp(u):
            starts = dw_dst[u]
            wd = BLK // len(starts)
            return [pltpu.make_async_copy(WR.at[u, :, :, pl.ds(wd * i, wd)], dw_out.at[:, :, pl.ds(al(s, LN), wd)], kc_l.at[2 * (u // 2) + (u % 2) * (u // 2) + u % 2 + i])
                    for i, s in enumerate(starts)]

        def dw_final(u):
            for q, d in enumerate(DT):
                if d[0] == u:
                    det(2, q).wait_recv()
            for q, d in enumerate(ZX):
                if d[0] == u:
                    zx(q).wait_recv()

            def add(q, carry):
                WR[u, q] += W[u, q]
                return carry

            lax.fori_loop(0, TAPS, add, 0)
            for o in dw_out_cp(u):
                o.start()

        dw_steps(0, 0, 4)
        dw_send(0)
        g_sib.wait_recv()
        dw_steps(1, 0, 4)
        dw_send(1)
        da_unit(0)
        da_unit(1)

        def last(n, carry):
            v = ACC[pl.ds(2 * n, 2)].reshape(448, BLK) + da_rows(3, n)
            v = v.astype(BF).reshape(2, HW, NB, BLK)
            for s in range(4):
                DAO[s, pl.ds(2 * n, 2)] = v[:, :, 2 * s:2 * s + 2, :]
            for s in range(4):
                da_copy(s, n).start()
            return carry

        def arrive(u, lo, hi):
            for c in range(lo, hi):
                if u == 3 and c < GX:
                    gdet(2, c).wait_recv()
                else:
                    g_x(u, c).wait_recv()
                g_rel(u, c, mine).start()
            for c in range(lo, hi):
                g_rel(u, c, theirs).wait_recv()

        arrive(2, 0, 4)
        dw_steps(2, 0, 2)
        arrive(2, 4, 6)
        dw_steps(2, 2, 3)
        for c in range(CH):
            g_x(2, c).wait_send()
        for c in range(GX, CH):
            g_x(3, c).start()
        arrive(2, 6, 7)
        dw_steps(2, 3, 4)
        dw_send(2)
        da_unit(2)
        arrive(3, 0, 4)

        @pl.when(k == 0)
        def _():
            lax.fori_loop(0, 7, last, 0)

        dw_steps(3, 0, 2)
        dw_final(0)
        arrive(3, 4, 6)
        dw_steps(3, 2, 3)

        @pl.when(k == 1)
        def _():
            lax.fori_loop(0, 4, last, 0)

        arrive(3, 6, 7)
        dw_steps(3, 3, 4)
        dw_send(3)

        @pl.when(k == 1)
        def _():
            lax.fori_loop(4, 7, last, 0)

        dw_final(1)
        for u in range(2, 4):
            dw_final(u)

        z_cp.wait()
        for u in range(4):
            for o in dw_out_cp(u):
                o.wait()
        for q in range(4):
            det(0, q).wait_send()
        for q in range(5):
            zx(q).wait_send()
        k_copy(1, pz, t).wait_send()
        k_z(pz).wait_send()
        k_copy(0, sib, t).wait_send()
        for i, (u, lane, wd, src) in enumerate(kc_pieces(sib, t)):
            remote(w.at[:, :, pl.ds(al(src, LN), wd)], KCU.at[u, :, pl.ds(al(LN * k, LN), LN), pl.ds(lane, wd)],
                   kc_s.at[i], kc_r.at[i], tp=sib).wait_send()
        for c in range(CH):
            for kind in range(3):
                if kind != 1 or c < CX:
                    a_fwd(kind, c).wait_send()
            g_rel(2, c, mine).wait_send()
            g_rel(3, c, mine).wait_send()
            if c < GX:
                gdet(0, c).wait_send()
            else:
                g_x(3, c).wait_send()
        g_sib.wait_send()
        for s in range(4):
            for n in range(7):
                da_copy(s, n).wait_send()


def solution(mesh):
    V = pltpu.VMEM
    D = pltpu.SemaphoreType.DMA
    any_spec = pl.BlockSpec(memory_space=pl.ANY)
    vm_spec = pl.BlockSpec(memory_space=pltpu.VMEM)
    call = pl.pallas_call(
        kernel,
        out_shape=[jax.ShapeDtypeStruct((HW, HW, NB, BLK), BF), jax.ShapeDtypeStruct((HW, HW, 2, CIN), BF), jax.ShapeDtypeStruct((TAPS, LN, 1024), F32)],
        in_specs=[any_spec, any_spec, vm_spec, vm_spec, any_spec],
        out_specs=[any_spec] * 3,
        scratch_shapes=[
            V((HP, HP, NB, CIN), BF), V((HP, HP, NB, LN), BF), V((TAPS, CIN, BLK), BF), V((4, TAPS, BLK, BLK), BF), V((4, 2304, BLK), BF),
            V((HW, HW, NB, BLK), BF), V((4, HP, HP, NB, BLK), BF), V((4, TAPS, LN, BLK), F32), V((4, TAPS, LN, BLK), F32),
            V((14, RW, BLK), F32), V((4, 14, HW, 2, BLK), BF), V((7, HW, 2, CIN), BF), V((4, HW, HW, 2, CIN), BF), V((2, HW, HW, 2, BLK), BF),
            D((2,)), D((3,)), D((3,)), D((6,)), D((6,)), D((6,)), D((CH,)), D((2,)), D((2,)), D((2,)), D((4, CH)), D((3, CH)), D((1,)), D((1,)),
            D((2, CH)), D((2, CH)), D((3, GX)), D((3, GX)), D((2, CH)), D((2, CH)), D((5,)), D((5,)), D((3, 4)), D((3, 4)), D((4, 7)), D((4, 7)), D((5,)),
        ],
        compiler_params=pltpu.CompilerParams(collective_id=0, has_side_effects=True, vmem_limit_bytes=66000000),
        name="conv_block",
    )

    def body(act_loc, w_loc, scale_loc, shift_loc, grad_loc):
        z, da, dw = call(act_loc[0].transpose(1, 2, 0, 3), w_loc[0].reshape(TAPS, LN, 1024), scale_loc, shift_loc, grad_loc[0].transpose(1, 2, 0, 3))
        return z.transpose(2, 0, 1, 3)[None], da.transpose(2, 0, 1, 3)[None], dw.reshape(1, 3, 3, LN, 1024)

    act_spec = P("stage", ("dp", "tp"))
    w_spec = P("stage", None, None, "tp")
    vec_spec = P("stage", "tp")
    grad_spec = P("stage", "dp", None, None, "tp")
    return jax.shard_map(body, mesh=mesh, in_specs=(act_spec, w_spec, vec_spec, vec_spec, grad_spec), out_specs=(grad_spec, act_spec, w_spec), check_vma=False)
```

```python
import functools

import jax
import jax.numpy as jnp
from jax import lax
from jax.experimental import pallas as pl
from jax.experimental.pallas import tpu as pltpu
from jax.sharding import PartitionSpec as P

BF = jnp.bfloat16
F32 = jnp.float32
MESH = pl.DeviceIdType.MESH
CH = 7
CB = (0, 5, 9, 13, 17, 21, 25, 28)
GR = 4
CX = 5
GX = 4
DT = ((1, 0), (1, 1), (1, 2), (2, 2))
ZX = ((0, 0, 9), (2, 0, 6), (3, 0, 3), (3, 3, 3), (3, 6, 3))
HW = 28
HP = 30
NB = 8
RW = 224
TAPS = 9
LN = 128
BLK = 256
CIN = 512


def kernel(act, w, sc, sh, gz, z_out, da_out, dw_out, A, AC, KO, KCU, KT, DZ, GU, W, WR, ACC, DAO, ZB,
           lsem, ksem_s, ksem_r, kx_s, kx_r, kz_s, kz_r, kc_s, kc_r, kc_l, as_s, ax_s, ax_r, af_s, a_r, f_s, gs_s, gs_r, g_s, g_r, gd_s, gd_r, rel_s, rel_r,
           zx_s, zx_r, d_s, d_r, da_s, da_r, out_s):
    dp = lax.axis_index("dp")
    stage = lax.axis_index("stage")
    t = lax.axis_index("tp")
    x = t // 2
    k = t % 2
    sib = x * 2 + (1 - k)
    xn = (1 - x) * 2 + k
    dg = (1 - x) * 2 + (1 - k)
    pz = (1 - x) * 2 + (k + dp) % 2
    pz2 = (1 - x) * 2 + (k + 1 - dp) % 2
    base = (1 - x) * CIN

    def al(v, m):
        return pl.multiple_of(v, m)

    def remote(src, dst, ssem, rsem, **dev):
        return pltpu.make_async_remote_copy(src_ref=src, dst_ref=dst, send_sem=ssem, recv_sem=rsem, device_id=dev, device_id_type=MESH)

    A[0] = jnp.zeros((HP, NB, CIN), BF)
    A[29] = jnp.zeros((HP, NB, CIN), BF)
    A[:, 0] = jnp.zeros((HP, NB, CIN), BF)
    A[:, 29] = jnp.zeros((HP, NB, CIN), BF)

    def zero_halo(u, carry):
        GU[u, 0] = jnp.zeros((HP, NB, BLK), BF)
        GU[u, 29] = jnp.zeros((HP, NB, BLK), BF)
        GU[u, :, 0] = jnp.zeros((HP, NB, BLK), BF)
        GU[u, :, 29] = jnp.zeros((HP, NB, BLK), BF)
        return carry

    lax.fori_loop(0, 4, zero_halo, 0)

    barrier = pltpu.get_barrier_semaphore()
    for ds in range(2):
        for dt in range(4):
            if ds or dt:
                pl.semaphore_signal(barrier, inc=1, device_id={"stage": (stage + ds) % 2, "tp": (t + dt) % 4}, device_id_type=MESH)
    pl.semaphore_signal(barrier, inc=1, device_id={"dp": 1 - dp}, device_id_type=MESH)
    pl.semaphore_wait(barrier, NB)

    def k_slot(src_tp):
        return KO.at[:, pl.ds(al(LN * src_tp, LN), LN), :]

    def k_copy(rel, peer, src_tp):
        return remote(w.at[:, :, pl.ds(al(BLK * peer, BLK), BLK)], k_slot(src_tp), ksem_s.at[rel], ksem_r.at[rel], tp=peer)

    def k_x(peer, src_tp, p):
        taps = pl.ds(3 * p, 3)
        return remote(w.at[taps, :, pl.ds(al(BLK * peer, BLK), BLK)], KO.at[taps, pl.ds(al(LN * src_tp, LN), LN), :], kx_s.at[p], kx_r.at[p], tp=peer)

    def k_z(src_tp, p):
        slot = KO.at[pl.ds(3 * p, 3), pl.ds(al(LN * src_tp, LN), LN), :]
        return remote(slot, slot, kz_s.at[p], kz_r.at[p], dp=1 - dp)

    def kc_pieces(own, other):
        return ((0, 0, BLK, BLK * own), (1, 0, BLK, BLK * other), (2, 0, LN, base), (2, LN, LN, base + BLK),
                (3, 0, LN, base + LN), (3, LN, LN, base + 384))

    def a_slot(src, c):
        return A.at[pl.ds(1 + CB[c], CB[c + 1] - CB[c]), pl.ds(1, HW), pl.ds(2 * src, 2), :]

    def a_direct(c):
        return remote(act.at[pl.ds(CB[c], CB[c + 1] - CB[c])], a_slot(t, c), as_s.at[c], a_r.at[3, c], stage=1)

    def a_cross(c):
        return remote(act.at[pl.ds(CB[c], CB[c + 1] - CB[c])], a_slot(t, c), ax_s.at[c - CX], ax_r.at[c - CX], tp=xn)

    def a_cross_fwd(c):
        return remote(a_slot(xn, c), a_slot(xn, c), af_s.at[c - CX], a_r.at[1, c], stage=1)

    def a_fwd(kind, c):
        if kind == 0:
            return remote(a_slot(t, c), a_slot(t, c), f_s.at[0, c], a_r.at[0, c], tp=sib)
        if kind == 1:
            return remote(a_slot(t, c), a_slot(t, c), f_s.at[1, c], a_r.at[1, c], tp=xn)
        return remote(a_slot(xn, c), a_slot(xn, c), f_s.at[2, c], a_r.at[2, c], tp=sib)

    def a_recv(rel, src, c):
        return remote(a_slot(src, c), a_slot(src, c), f_s.at[0, c], a_r.at[rel, c], tp=sib)

    def g_rows(u, r0, n, lane, width):
        return GU.at[u, pl.ds(1 + r0, n), pl.ds(1, HW), :, pl.ds(lane, width)]

    mine = al(LN * k, LN)
    theirs = al(LN * (1 - k), LN)

    def g_x(u, c):
        return remote(g_rows(0, GR * c, GR, LN * (u - 2), LN), g_rows(u, GR * c, GR, mine, LN), g_s.at[u - 2, c], g_r.at[u - 2, c], tp=xn)

    def g_rel(u, c, lane):
        return remote(g_rows(u, GR * c, GR, lane, LN), g_rows(u, GR * c, GR, lane, LN), rel_s.at[u - 2, c], rel_r.at[u - 2, c], tp=sib)

    def gdet(leg, c):
        own = g_rows(0, GR * c, GR, LN, LN)
        a3 = g_rows(3, GR * c, GR, mine, LN)
        a2 = g_rows(2, GR * c, GR, mine, LN)
        src, dst, dev = ((own, a3, {"stage": 0}), (a3, a2, {"tp": xn}), (a2, a3, {"stage": 1}))[leg]
        return remote(src, dst, gd_s.at[leg, c], gd_r.at[leg, c], **dev)

    def det(leg, q):
        src, dst = ((W, WR), (WR, W), (W, WR))[leg]
        dev = ({"stage": 0}, {"dp": 1 - dp}, {"stage": 1})[leg]
        u, p = DT[q]
        return remote(src.at[u, pl.ds(3 * p, 3)], dst.at[u, pl.ds(3 * p, 3)], d_s.at[leg, q], d_r.at[leg, q], **dev)

    def zx(q):
        u, p, n = ZX[q]
        return remote(W.at[u, pl.ds(p, n)], WR.at[u, pl.ds(p, n)], zx_s.at[q], zx_r.at[q], dp=1 - dp)

    def da_copy(s, n):
        return remote(DAO.at[pl.ds(2 * n, 2), :, pl.ds(2 * s, 2), :],
                      da_out.at[pl.ds(14 * k + 2 * n, 2), :, :, pl.ds(al(BLK * x, BLK), BLK)],
                      da_s.at[s, n], da_r.at[t, n], stage=0, tp=s)

    @pl.when(stage == 0)
    def _():
        for c in range(CX, CH):
            a_cross(c).start()
        for c in range(CH):
            a_direct(c).start()
        for c in range(CX, CH):
            a_cross(c).wait_recv()
            a_cross_fwd(c).start()
        W[0] = jnp.zeros((TAPS, LN, BLK), F32)

        def zrow(h, carry):
            DZ[h] = jnp.zeros((HW, NB, BLK), BF)
            return carry

        lax.fori_loop(0, HW, zrow, 0)
        outs = [pltpu.make_async_copy(W.at[0], dw_out.at[:, :, pl.ds(BLK * u, BLK)], out_s.at[u]) for u in range(4)]
        outs.append(pltpu.make_async_copy(DZ, z_out, out_s.at[4]))
        for o in outs:
            o.start()
        for o in outs:
            o.wait()
        for c in range(GX):
            gdet(0, c).wait_recv()
            gdet(1, c).start()
        for c in range(CH):
            a_direct(c).wait_send()
        for c in range(CX, CH):
            a_cross(c).wait_send()
            a_cross_fwd(c).wait_send()
        for c in range(GX):
            gdet(1, c).wait_recv()
            gdet(2, c).start()
        for leg, q in ((0, 0), (0, 1), (1, 0), (0, 2), (1, 1), (1, 2), (0, 3), (1, 3)):
            det(leg, q).wait_recv()
            det(leg + 1, q).start()
        for q in range(4):
            det(1, q).wait_send()
            det(2, q).wait_send()
        for c in range(GX):
            gdet(1, c).wait_send()
            gdet(2, c).wait_send()
        for src in range(4):
            for n in range(7):
                remote(DAO.at[pl.ds(2 * n, 2), :, pl.ds(0, 2), :],
                       da_out.at[pl.ds(14 * (src % 2) + 2 * n, 2), :, :, pl.ds(BLK * (src // 2), BLK)],
                       da_s.at[0, n], da_r.at[src, n], stage=0, tp=0).wait_recv()

    @pl.when(stage == 1)
    def _():
        for p in range(3):
            k_x(pz, t, p).start()
        k_copy(0, sib, t).start()
        for i, (u, lane, wd, src) in enumerate(kc_pieces(sib, t)):
            remote(w.at[:, :, pl.ds(al(src, LN), wd)], KCU.at[u, :, pl.ds(al(LN * k, LN), LN), pl.ds(lane, wd)],
                   kc_s.at[i], kc_r.at[i], tp=sib).start()
        loc = [pltpu.make_async_copy(w.at[:, :, pl.ds(al(src, LN), wd)], KCU.at[u, :, pl.ds(al(LN * k, LN), LN), pl.ds(lane, wd)], kc_l.at[i])
               for i, (u, lane, wd, src) in enumerate(kc_pieces(t, sib))]
        loc.append(pltpu.make_async_copy(w.at[:, :, pl.ds(al(BLK * t, BLK), BLK)], KO.at[:, pl.ds(al(LN * t, LN), LN), :], lsem.at[0]))
        loc.append(pltpu.make_async_copy(gz, DZ, lsem.at[1]))
        for o in loc:
            o.start()
        ZB[...] = jnp.zeros((7, HW, 2, CIN), BF)
        zcp = [pltpu.make_async_copy(ZB, da_out.at[pl.ds(7 * i, 7)], out_s.at[i]) for i in range(4)]
        for o in zcp:
            o.start()
        ACC[...] = jnp.zeros((14, RW, BLK), F32)
        W[...] = jnp.zeros((4, TAPS, LN, BLK), F32)
        AC[0] = jnp.zeros((HP, NB, LN), BF)
        AC[29] = jnp.zeros((HP, NB, LN), BF)

        def forward_images(c):
            a_recv(3, t, c).wait_recv()
            if c < CX:
                a_fwd(1, c).start()
            a_fwd(0, c).start()

        def transpose(u):
            def tr(tap, carry):
                KT[u, pl.ds(tap * BLK, BLK)] = KCU[u, tap].T
                return carry

            lax.fori_loop(0, TAPS, tr, 0)

        def weights_on(p):
            k_x(t, pz, p).wait_recv()
            k_z(pz, p).start()

        weights_on(0)
        forward_images(0)
        weights_on(1)
        for o in loc:
            o.wait()
        for o in zcp:
            o.wait()
        for i, (u, lane, wd, src) in enumerate(kc_pieces(t, sib)):
            remote(w.at[:, :, pl.ds(al(src, LN), wd)], KCU.at[u, :, pl.ds(theirs, LN), pl.ds(lane, wd)],
                   kc_s.at[i], kc_r.at[i], tp=sib).wait_recv()
        transpose(0)
        forward_images(1)
        weights_on(2)
        transpose(1)
        transpose(2)
        forward_images(2)
        transpose(3)

        def row(h, carry):
            lhs = jnp.concatenate([A[h + i, j:j + HW].reshape(RW, CIN) for i in range(3) for j in range(3)], axis=1)
            pre = jnp.dot(lhs, KO[...].reshape(4608, BLK), preferred_element_type=F32)
            y = pre * sc[...] + sh[...]
            d = DZ[h].reshape(RW, BLK).astype(F32)
            g = jnp.where(y > 0, d * sc[...], 0.0).astype(BF)
            DZ[h] = jnp.maximum(y, 0.0).astype(BF).reshape(HW, NB, BLK)
            GU[0, h + 1, 1:29] = g.reshape(HW, NB, BLK)
            return carry

        z_cp = pltpu.make_async_copy(DZ, z_out, lsem.at[0])
        g_sib = remote(GU.at[0], GU.at[1], gs_s.at[0], gs_r.at[0], tp=sib)

        for c in range(CH):
            if c + 3 < CH:
                forward_images(c + 3)
            if c == 0:
                for p in range(3):
                    k_z(pz2, p).wait_recv()
                k_copy(0, t, sib).wait_recv()
            a_recv(1, xn, c).wait_recv()
            a_fwd(2, c).start()
            a_recv(0, sib, c).wait_recv()
            a_recv(2, dg, c).wait_recv()
            new = pl.ds(1 + CB[c], CB[c + 1] - CB[c])
            AC[new] = A[new, :, :, pl.ds(al(LN * t, LN), LN)]
            lax.fori_loop(GR * c, GR * c + GR, row, 0)
            if c < GX:
                gdet(0, c).start()
            if c == 1:
                g_x(2, 0).start()
            if c > 0:
                g_x(2, c).start()
        g_sib.start()
        z_cp.start()

        def dw_step(u, n):
            h = n * 7
            lhs = jnp.concatenate([AC[pl.ds(h + i, 7), j:j + HW].reshape(1568, LN) for i in range(3) for j in range(3)], axis=1)
            rhs = GU[u, pl.ds(h + 1, 7), 1:29].reshape(1568, BLK)
            p = lax.dot_general(lhs, rhs, (((0,), (0,)), ((), ())), preferred_element_type=F32)
            W[u] += p.reshape(TAPS, LN, BLK)

        def dw_steps(u, lo, hi):
            def step(n, carry):
                dw_step(u, n)
                return carry

            lax.fori_loop(lo, hi, step, 0)

        def dw_send(u):
            for q, d in enumerate(DT):
                if d[0] == u:
                    det(0, q).start()
            for q, d in enumerate(ZX):
                if d[0] == u:
                    zx(q).start()

        def da_rows(u, n):
            h = 14 * k + 2 * n
            lhs = jnp.concatenate([GU[u, pl.ds(h + 2 - i, 2), 2 - j:HP - j].reshape(448, BLK) for i in range(3) for j in range(3)], axis=1)
            return jnp.dot(lhs, KT[u], preferred_element_type=F32)

        def da_unit(u, count=7):
            def step(n, carry):
                ACC[pl.ds(2 * n, 2)] += da_rows(u, n).reshape(2, RW, BLK)
                return carry

            lax.fori_loop(0, count, step, 0)

        dw_dst = ((BLK * t,), (BLK * sib,), (base, base + BLK), (base + LN, base + 384))

        def dw_out_cp(u):
            starts = dw_dst[u]
            wd = BLK // len(starts)
            return [pltpu.make_async_copy(WR.at[u, :, :, pl.ds(wd * i, wd)], dw_out.at[:, :, pl.ds(al(s, LN), wd)], kc_l.at[2 * (u // 2) + (u % 2) * (u // 2) + u % 2 + i])
                    for i, s in enumerate(starts)]

        def dw_final(u):
            for q, d in enumerate(DT):
                if d[0] == u:
                    det(2, q).wait_recv()
            for q, d in enumerate(ZX):
                if d[0] == u:
                    zx(q).wait_recv()

            def add(q, carry):
                WR[u, q] += W[u, q]
                return carry

            lax.fori_loop(0, TAPS, add, 0)
            for o in dw_out_cp(u):
                o.start()

        dw_steps(0, 0, 4)
        dw_send(0)
        g_sib.wait_recv()
        dw_steps(1, 0, 4)
        dw_send(1)
        da_unit(0)

        def last(n, carry):
            v = ACC[pl.ds(2 * n, 2)].reshape(448, BLK) + da_rows(3, n)
            DAO[pl.ds(2 * n, 2)] = v.astype(BF).reshape(2, HW, NB, BLK)
            for s in range(4):
                da_copy(s, n).start()
            return carry

        def take(u, lo, hi):
            for c in range(lo, hi):
                if u == 3 and c < GX:
                    gdet(2, c).wait_recv()
                else:
                    g_x(u, c).wait_recv()
                g_rel(u, c, mine).start()

        def got(u, lo, hi):
            for c in range(lo, hi):
                g_rel(u, c, theirs).wait_recv()

        take(2, 0, 6)
        got(2, 0, 6)
        dw_steps(2, 0, 3)
        for c in range(CH):
            g_x(2, c).wait_send()
        for c in range(GX, CH):
            g_x(3, c).start()
        take(2, 6, 7)
        got(2, 6, 7)
        dw_steps(2, 3, 4)
        dw_send(2)
        take(3, 0, 4)
        got(3, 0, 4)
        dw_steps(3, 0, 2 * k)
        da_unit(1)
        da_unit(2, 7 - 7 * k)
        take(3, 4, 7)
        lax.fori_loop(0, 7 - 7 * k, last, 0)
        got(3, 4, 7)
        dw_steps(3, 2 * k, 4)
        dw_send(3)
        da_unit(2, 7 * k)
        lax.fori_loop(0, 7 * k, last, 0)
        dw_final(0)
        dw_final(1)
        for u in range(2, 4):
            dw_final(u)

        z_cp.wait()
        for u in range(4):
            for o in dw_out_cp(u):
                o.wait()
        for q in range(4):
            det(0, q).wait_send()
        for q in range(5):
            zx(q).wait_send()
        for p in range(3):
            k_x(pz, t, p).wait_send()
            k_z(pz, p).wait_send()
        k_copy(0, sib, t).wait_send()
        for i, (u, lane, wd, src) in enumerate(kc_pieces(sib, t)):
            remote(w.at[:, :, pl.ds(al(src, LN), wd)], KCU.at[u, :, pl.ds(al(LN * k, LN), LN), pl.ds(lane, wd)],
                   kc_s.at[i], kc_r.at[i], tp=sib).wait_send()
        for c in range(CH):
            for kind in range(3):
                if kind != 1 or c < CX:
                    a_fwd(kind, c).wait_send()
            g_rel(2, c, mine).wait_send()
            g_rel(3, c, mine).wait_send()
            if c < GX:
                gdet(0, c).wait_send()
            else:
                g_x(3, c).wait_send()
        g_sib.wait_send()
        for s in range(4):
            for n in range(7):
                da_copy(s, n).wait_send()


def solution(mesh):
    V = pltpu.VMEM
    D = pltpu.SemaphoreType.DMA
    any_spec = pl.BlockSpec(memory_space=pl.ANY)
    vm_spec = pl.BlockSpec(memory_space=pltpu.VMEM)
    call = pl.pallas_call(
        kernel,
        out_shape=[jax.ShapeDtypeStruct((HW, HW, NB, BLK), BF), jax.ShapeDtypeStruct((HW, HW, 2, CIN), BF), jax.ShapeDtypeStruct((TAPS, LN, 1024), F32)],
        in_specs=[any_spec, any_spec, vm_spec, vm_spec, any_spec],
        out_specs=[any_spec] * 3,
        scratch_shapes=[
            V((HP, HP, NB, CIN), BF), V((HP, HP, NB, LN), BF), V((TAPS, CIN, BLK), BF), V((4, TAPS, BLK, BLK), BF), V((4, 2304, BLK), BF),
            V((HW, HW, NB, BLK), BF), V((4, HP, HP, NB, BLK), BF), V((4, TAPS, LN, BLK), F32), V((4, TAPS, LN, BLK), F32),
            V((14, RW, BLK), F32), V((14, HW, NB, BLK), BF), V((7, HW, 2, CIN), BF),
            D((2,)), D((3,)), D((3,)), D((3,)), D((3,)), D((3,)), D((3,)), D((6,)), D((6,)), D((6,)), D((CH,)), D((2,)), D((2,)), D((2,)), D((4, CH)), D((3, CH)), D((1,)), D((1,)),
            D((2, CH)), D((2, CH)), D((3, GX)), D((3, GX)), D((2, CH)), D((2, CH)), D((5,)), D((5,)), D((3, 4)), D((3, 4)), D((4, 7)), D((4, 7)), D((5,)),
        ],
        compiler_params=pltpu.CompilerParams(collective_id=0, has_side_effects=True, vmem_limit_bytes=66000000),
        name="conv_block",
    )

    def body(act_loc, w_loc, scale_loc, shift_loc, grad_loc):
        z, da, dw = call(act_loc[0].transpose(1, 2, 0, 3), w_loc[0].reshape(TAPS, LN, 1024), scale_loc, shift_loc, grad_loc[0].transpose(1, 2, 0, 3))
        return z.transpose(2, 0, 1, 3)[None], da.transpose(2, 0, 1, 3)[None], dw.reshape(1, 3, 3, LN, 1024)

    act_spec = P("stage", ("dp", "tp"))
    w_spec = P("stage", None, None, "tp")
    vec_spec = P("stage", "tp")
    grad_spec = P("stage", "dp", None, None, "tp")
    return jax.shard_map(body, mesh=mesh, in_specs=(act_spec, w_spec, vec_spec, vec_spec, grad_spec), out_specs=(grad_spec, act_spec, w_spec), check_vma=False)
```

```python
import functools

import jax
import jax.numpy as jnp
from jax import lax
from jax.experimental import pallas as pl
from jax.experimental.pallas import tpu as pltpu
from jax.sharding import PartitionSpec as P

BF = jnp.bfloat16
F32 = jnp.float32
MESH = pl.DeviceIdType.MESH
CH = 7
CB = (0, 5, 9, 13, 17, 21, 25, 28)
GR = 4
CX = 5
GX = 4
DT = ((1, 0), (1, 1), (1, 2), (2, 2))
ZX = ((0, 0, 9), (2, 0, 6), (3, 0, 3), (3, 3, 3), (3, 6, 3))
HW = 28
HP = 30
NB = 8
RW = 224
TAPS = 9
LN = 128
BLK = 256
CIN = 512


def kernel(act, w, sc, sh, gz, z_out, da_out, dw_out, A, AC, KO, KCU, KT, DZ, GU, W, WR, ACC, DAO, ZB,
           lsem, ksem_s, ksem_r, kx_s, kx_r, kz_s, kz_r, kc_s, kc_r, kc_l, as_s, ax_s, ax_r, af_s, a_r, f_s, gs_s, gs_r, g_s, g_r, gd_s, gd_r, rel_s, rel_r,
           zx_s, zx_r, d_s, d_r, da_s, da_r, out_s):
    dp = lax.axis_index("dp")
    stage = lax.axis_index("stage")
    t = lax.axis_index("tp")
    x = t // 2
    k = t % 2
    sib = x * 2 + (1 - k)
    xn = (1 - x) * 2 + k
    dg = (1 - x) * 2 + (1 - k)
    pz = (1 - x) * 2 + (k + dp) % 2
    pz2 = (1 - x) * 2 + (k + 1 - dp) % 2
    base = (1 - x) * CIN

    def al(v, m):
        return pl.multiple_of(v, m)

    def remote(src, dst, ssem, rsem, **dev):
        return pltpu.make_async_remote_copy(src_ref=src, dst_ref=dst, send_sem=ssem, recv_sem=rsem, device_id=dev, device_id_type=MESH)

    A[0] = jnp.zeros((HP, NB, CIN), BF)
    A[29] = jnp.zeros((HP, NB, CIN), BF)
    A[:, 0] = jnp.zeros((HP, NB, CIN), BF)
    A[:, 29] = jnp.zeros((HP, NB, CIN), BF)

    def zero_halo(u, carry):
        GU[u, 0] = jnp.zeros((HP, NB, BLK), BF)
        GU[u, 29] = jnp.zeros((HP, NB, BLK), BF)
        GU[u, :, 0] = jnp.zeros((HP, NB, BLK), BF)
        GU[u, :, 29] = jnp.zeros((HP, NB, BLK), BF)
        return carry

    lax.fori_loop(0, 4, zero_halo, 0)

    barrier = pltpu.get_barrier_semaphore()
    for ds in range(2):
        for dt in range(4):
            if ds or dt:
                pl.semaphore_signal(barrier, inc=1, device_id={"stage": (stage + ds) % 2, "tp": (t + dt) % 4}, device_id_type=MESH)
    pl.semaphore_signal(barrier, inc=1, device_id={"dp": 1 - dp}, device_id_type=MESH)
    pl.semaphore_wait(barrier, NB)

    def k_slot(src_tp):
        return KO.at[:, pl.ds(al(LN * src_tp, LN), LN), :]

    def k_copy(rel, peer, src_tp):
        return remote(w.at[:, :, pl.ds(al(BLK * peer, BLK), BLK)], k_slot(src_tp), ksem_s.at[rel], ksem_r.at[rel], tp=peer)

    def k_x(peer, src_tp, p):
        taps = pl.ds(3 * p, 3)
        return remote(w.at[taps, :, pl.ds(al(BLK * peer, BLK), BLK)], KO.at[taps, pl.ds(al(LN * src_tp, LN), LN), :], kx_s.at[p], kx_r.at[p], tp=peer)

    def k_z(src_tp, p):
        slot = KO.at[pl.ds(3 * p, 3), pl.ds(al(LN * src_tp, LN), LN), :]
        return remote(slot, slot, kz_s.at[p], kz_r.at[p], dp=1 - dp)

    def kc_pieces(own, other):
        return ((0, 0, BLK, BLK * own), (1, 0, BLK, BLK * other), (2, 0, LN, base), (2, LN, LN, base + BLK),
                (3, 0, LN, base + LN), (3, LN, LN, base + 384))

    def a_slot(src, c):
        return A.at[pl.ds(1 + CB[c], CB[c + 1] - CB[c]), pl.ds(1, HW), pl.ds(2 * src, 2), :]

    def a_direct(c):
        return remote(act.at[pl.ds(CB[c], CB[c + 1] - CB[c])], a_slot(t, c), as_s.at[c], a_r.at[3, c], stage=1)

    def a_cross(c):
        return remote(act.at[pl.ds(CB[c], CB[c + 1] - CB[c])], a_slot(t, c), ax_s.at[c - CX], ax_r.at[c - CX], tp=xn)

    def a_cross_fwd(c):
        return remote(a_slot(xn, c), a_slot(xn, c), af_s.at[c - CX], a_r.at[1, c], stage=1)

    def a_fwd(kind, c):
        if kind == 0:
            return remote(a_slot(t, c), a_slot(t, c), f_s.at[0, c], a_r.at[0, c], tp=sib)
        if kind == 1:
            return remote(a_slot(t, c), a_slot(t, c), f_s.at[1, c], a_r.at[1, c], tp=xn)
        return remote(a_slot(xn, c), a_slot(xn, c), f_s.at[2, c], a_r.at[2, c], tp=sib)

    def a_recv(rel, src, c):
        return remote(a_slot(src, c), a_slot(src, c), f_s.at[0, c], a_r.at[rel, c], tp=sib)

    def g_rows(u, r0, n, lane, width):
        return GU.at[u, pl.ds(1 + r0, n), pl.ds(1, HW), :, pl.ds(lane, width)]

    mine = al(LN * k, LN)
    theirs = al(LN * (1 - k), LN)

    def g_x(u, c):
        return remote(g_rows(0, GR * c, GR, LN * (u - 2), LN), g_rows(u, GR * c, GR, mine, LN), g_s.at[u - 2, c], g_r.at[u - 2, c], tp=xn)

    def g_rel(u, c, lane):
        return remote(g_rows(u, GR * c, GR, lane, LN), g_rows(u, GR * c, GR, lane, LN), rel_s.at[u - 2, c], rel_r.at[u - 2, c], tp=sib)

    def gdet(leg, c):
        own = g_rows(0, GR * c, GR, LN, LN)
        a3 = g_rows(3, GR * c, GR, mine, LN)
        a2 = g_rows(2, GR * c, GR, mine, LN)
        src, dst, dev = ((own, a3, {"stage": 0}), (a3, a2, {"tp": xn}), (a2, a3, {"stage": 1}))[leg]
        return remote(src, dst, gd_s.at[leg, c], gd_r.at[leg, c], **dev)

    def det(leg, q):
        src, dst = ((W, WR), (WR, W), (W, WR))[leg]
        dev = ({"stage": 0}, {"dp": 1 - dp}, {"stage": 1})[leg]
        u, p = DT[q]
        return remote(src.at[u, pl.ds(3 * p, 3)], dst.at[u, pl.ds(3 * p, 3)], d_s.at[leg, q], d_r.at[leg, q], **dev)

    def zx(q):
        u, p, n = ZX[q]
        return remote(W.at[u, pl.ds(p, n)], WR.at[u, pl.ds(p, n)], zx_s.at[q], zx_r.at[q], dp=1 - dp)

    def da_copy(s, n):
        return remote(DAO.at[pl.ds(2 * n, 2), :, pl.ds(2 * s, 2), :],
                      da_out.at[pl.ds(14 * k + 2 * n, 2), :, :, pl.ds(al(BLK * x, BLK), BLK)],
                      da_s.at[s, n], da_r.at[t, n], stage=0, tp=s)

    @pl.when(stage == 0)
    def _():
        for c in range(CX, CH):
            a_cross(c).start()
        for c in range(CH):
            a_direct(c).start()
        for c in range(CX, CH):
            a_cross(c).wait_recv()
            a_cross_fwd(c).start()
        W[0] = jnp.zeros((TAPS, LN, BLK), F32)

        def zrow(h, carry):
            DZ[h] = jnp.zeros((HW, NB, BLK), BF)
            return carry

        lax.fori_loop(0, HW, zrow, 0)
        outs = [pltpu.make_async_copy(W.at[0], dw_out.at[:, :, pl.ds(BLK * u, BLK)], out_s.at[u]) for u in range(4)]
        outs.append(pltpu.make_async_copy(DZ, z_out, out_s.at[4]))
        for o in outs:
            o.start()
        for o in outs:
            o.wait()
        for c in range(GX):
            gdet(0, c).wait_recv()
            gdet(1, c).start()
        for c in range(CH):
            a_direct(c).wait_send()
        for c in range(CX, CH):
            a_cross(c).wait_send()
            a_cross_fwd(c).wait_send()
        for c in range(GX):
            gdet(1, c).wait_recv()
            gdet(2, c).start()
        for leg, q in ((0, 0), (0, 1), (1, 0), (0, 2), (1, 1), (1, 2), (0, 3), (1, 3)):
            det(leg, q).wait_recv()
            det(leg + 1, q).start()
        for q in range(4):
            det(1, q).wait_send()
            det(2, q).wait_send()
        for c in range(GX):
            gdet(1, c).wait_send()
            gdet(2, c).wait_send()
        for src in range(4):
            for n in range(7):
                remote(DAO.at[pl.ds(2 * n, 2), :, pl.ds(0, 2), :],
                       da_out.at[pl.ds(14 * (src % 2) + 2 * n, 2), :, :, pl.ds(BLK * (src // 2), BLK)],
                       da_s.at[0, n], da_r.at[src, n], stage=0, tp=0).wait_recv()

    @pl.when(stage == 1)
    def _():
        for p in range(3):
            k_x(pz, t, p).start()
        k_copy(0, sib, t).start()
        for i, (u, lane, wd, src) in enumerate(kc_pieces(sib, t)):
            remote(w.at[:, :, pl.ds(al(src, LN), wd)], KCU.at[u, :, pl.ds(al(LN * k, LN), LN), pl.ds(lane, wd)],
                   kc_s.at[i], kc_r.at[i], tp=sib).start()
        loc = [pltpu.make_async_copy(w.at[:, :, pl.ds(al(src, LN), wd)], KCU.at[u, :, pl.ds(al(LN * k, LN), LN), pl.ds(lane, wd)], kc_l.at[i])
               for i, (u, lane, wd, src) in enumerate(kc_pieces(t, sib))]
        loc.append(pltpu.make_async_copy(w.at[:, :, pl.ds(al(BLK * t, BLK), BLK)], KO.at[:, pl.ds(al(LN * t, LN), LN), :], lsem.at[0]))
        loc.append(pltpu.make_async_copy(gz, DZ, lsem.at[1]))
        for o in loc:
            o.start()
        ZB[...] = jnp.zeros((7, HW, 2, CIN), BF)
        zcp = [pltpu.make_async_copy(ZB, da_out.at[pl.ds(7 * i, 7)], out_s.at[i]) for i in range(4)]
        for o in zcp:
            o.start()
        ACC[...] = jnp.zeros((14, RW, BLK), F32)
        W[...] = jnp.zeros((4, TAPS, LN, BLK), F32)
        AC[0] = jnp.zeros((HP, NB, LN), BF)
        AC[29] = jnp.zeros((HP, NB, LN), BF)

        def forward_images(c):
            a_recv(3, t, c).wait_recv()
            if c < CX:
                a_fwd(1, c).start()
            a_fwd(0, c).start()

        def transpose(u):
            def tr(tap, carry):
                KT[u, pl.ds(tap * BLK, BLK)] = KCU[u, tap].T
                return carry

            lax.fori_loop(0, TAPS, tr, 0)

        def weights_on(p):
            k_x(t, pz, p).wait_recv()
            k_z(pz, p).start()

        weights_on(0)
        forward_images(0)
        weights_on(1)
        for o in loc:
            o.wait()
        for o in zcp:
            o.wait()
        for i, (u, lane, wd, src) in enumerate(kc_pieces(t, sib)):
            remote(w.at[:, :, pl.ds(al(src, LN), wd)], KCU.at[u, :, pl.ds(theirs, LN), pl.ds(lane, wd)],
                   kc_s.at[i], kc_r.at[i], tp=sib).wait_recv()
        transpose(0)
        forward_images(1)
        weights_on(2)
        transpose(1)
        transpose(2)
        forward_images(2)
        transpose(3)

        def rows(m, carry):
            h = 2 * m
            two = pl.ds(h, 2)
            lhs = jnp.concatenate([A[pl.ds(h + i, 2), j:j + HW].reshape(2 * RW, CIN) for i in range(3) for j in range(3)], axis=1)
            pre = jnp.dot(lhs, KO[...].reshape(4608, BLK), preferred_element_type=F32)
            y = pre * sc[...] + sh[...]
            d = DZ[two].reshape(2 * RW, BLK).astype(F32)
            g = jnp.where(y > 0, d * sc[...], 0.0).astype(BF)
            DZ[two] = jnp.maximum(y, 0.0).astype(BF).reshape(2, HW, NB, BLK)
            GU[0, pl.ds(h + 1, 2), 1:29] = g.reshape(2, HW, NB, BLK)
            return carry

        z_cp = pltpu.make_async_copy(DZ, z_out, lsem.at[0])
        g_sib = remote(GU.at[0], GU.at[1], gs_s.at[0], gs_r.at[0], tp=sib)

        for c in range(CH):
            if c + 3 < CH:
                forward_images(c + 3)
            if c == 0:
                for p in range(3):
                    k_z(pz2, p).wait_recv()
                k_copy(0, t, sib).wait_recv()
            a_recv(1, xn, c).wait_recv()
            a_fwd(2, c).start()
            a_recv(0, sib, c).wait_recv()
            a_recv(2, dg, c).wait_recv()
            new = pl.ds(1 + CB[c], CB[c + 1] - CB[c])
            AC[new] = A[new, :, :, pl.ds(al(LN * t, LN), LN)]
            lax.fori_loop(2 * c, 2 * c + 2, rows, 0)
            if c < GX:
                gdet(0, c).start()
            if c == 1:
                g_x(2, 0).start()
            if c > 0:
                g_x(2, c).start()
        g_sib.start()
        z_cp.start()

        def dw_step(u, n):
            h = n * 7
            lhs = jnp.concatenate([AC[pl.ds(h + i, 7), j:j + HW].reshape(1568, LN) for i in range(3) for j in range(3)], axis=1)
            rhs = GU[u, pl.ds(h + 1, 7), 1:29].reshape(1568, BLK)
            p = lax.dot_general(lhs, rhs, (((0,), (0,)), ((), ())), preferred_element_type=F32)
            W[u] += p.reshape(TAPS, LN, BLK)

        def dw_steps(u, lo, hi):
            def step(n, carry):
                dw_step(u, n)
                return carry

            lax.fori_loop(lo, hi, step, 0)

        def dw_send(u):
            for q, d in enumerate(DT):
                if d[0] == u:
                    det(0, q).start()
            for q, d in enumerate(ZX):
                if d[0] == u:
                    zx(q).start()

        def da_rows(u, n):
            h = 14 * k + 2 * n
            lhs = jnp.concatenate([GU[u, pl.ds(h + 2 - i, 2), 2 - j:HP - j].reshape(448, BLK) for i in range(3) for j in range(3)], axis=1)
            return jnp.dot(lhs, KT[u], preferred_element_type=F32)

        def da_unit(u, count=7):
            def step(n, carry):
                ACC[pl.ds(2 * n, 2)] += da_rows(u, n).reshape(2, RW, BLK)
                return carry

            lax.fori_loop(0, count, step, 0)

        dw_dst = ((BLK * t,), (BLK * sib,), (base, base + BLK), (base + LN, base + 384))

        def dw_out_cp(u):
            starts = dw_dst[u]
            wd = BLK // len(starts)
            return [pltpu.make_async_copy(WR.at[u, :, :, pl.ds(wd * i, wd)], dw_out.at[:, :, pl.ds(al(s, LN), wd)], kc_l.at[2 * (u // 2) + (u % 2) * (u // 2) + u % 2 + i])
                    for i, s in enumerate(starts)]

        def dw_final(u):
            for q, d in enumerate(DT):
                if d[0] == u:
                    det(2, q).wait_recv()
            for q, d in enumerate(ZX):
                if d[0] == u:
                    zx(q).wait_recv()

            def add(q, carry):
                WR[u, q] += W[u, q]
                return carry

            lax.fori_loop(0, TAPS, add, 0)
            for o in dw_out_cp(u):
                o.start()

        dw_steps(0, 0, 4)
        dw_send(0)
        g_sib.wait_recv()
        dw_steps(1, 0, 4)
        dw_send(1)
        da_unit(0)

        def last(n, carry):
            v = ACC[pl.ds(2 * n, 2)].reshape(448, BLK) + da_rows(3, n)
            DAO[pl.ds(2 * n, 2)] = v.astype(BF).reshape(2, HW, NB, BLK)
            for s in range(4):
                da_copy(s, n).start()
            return carry

        def take(u, lo, hi):
            for c in range(lo, hi):
                if u == 3 and c < GX:
                    gdet(2, c).wait_recv()
                else:
                    g_x(u, c).wait_recv()
                g_rel(u, c, mine).start()

        def got(u, lo, hi):
            for c in range(lo, hi):
                g_rel(u, c, theirs).wait_recv()

        take(2, 0, 6)
        got(2, 0, 6)
        dw_steps(2, 0, 3)
        for c in range(CH):
            g_x(2, c).wait_send()
        for c in range(GX, CH):
            g_x(3, c).start()
        take(2, 6, 7)
        got(2, 6, 7)
        dw_steps(2, 3, 4)
        dw_send(2)
        take(3, 0, 4)
        got(3, 0, 4)
        dw_steps(3, 0, 2 * k)
        da_unit(1)
        da_unit(2, 7 - 7 * k)
        take(3, 4, 7)
        lax.fori_loop(0, 7 - 7 * k, last, 0)
        got(3, 4, 7)
        dw_steps(3, 2 * k, 4)
        dw_send(3)
        da_unit(2, 7 * k)
        lax.fori_loop(0, 7 * k, last, 0)
        dw_final(0)
        dw_final(1)
        for u in range(2, 4):
            dw_final(u)

        z_cp.wait()
        for u in range(4):
            for o in dw_out_cp(u):
                o.wait()
        for q in range(4):
            det(0, q).wait_send()
        for q in range(5):
            zx(q).wait_send()
        for p in range(3):
            k_x(pz, t, p).wait_send()
            k_z(pz, p).wait_send()
        k_copy(0, sib, t).wait_send()
        for i, (u, lane, wd, src) in enumerate(kc_pieces(sib, t)):
            remote(w.at[:, :, pl.ds(al(src, LN), wd)], KCU.at[u, :, pl.ds(al(LN * k, LN), LN), pl.ds(lane, wd)],
                   kc_s.at[i], kc_r.at[i], tp=sib).wait_send()
        for c in range(CH):
            for kind in range(3):
                if kind != 1 or c < CX:
                    a_fwd(kind, c).wait_send()
            g_rel(2, c, mine).wait_send()
            g_rel(3, c, mine).wait_send()
            if c < GX:
                gdet(0, c).wait_send()
            else:
                g_x(3, c).wait_send()
        g_sib.wait_send()
        for s in range(4):
            for n in range(7):
                da_copy(s, n).wait_send()


def solution(mesh):
    V = pltpu.VMEM
    D = pltpu.SemaphoreType.DMA
    any_spec = pl.BlockSpec(memory_space=pl.ANY)
    vm_spec = pl.BlockSpec(memory_space=pltpu.VMEM)
    call = pl.pallas_call(
        kernel,
        out_shape=[jax.ShapeDtypeStruct((HW, HW, NB, BLK), BF), jax.ShapeDtypeStruct((HW, HW, 2, CIN), BF), jax.ShapeDtypeStruct((TAPS, LN, 1024), F32)],
        in_specs=[any_spec, any_spec, vm_spec, vm_spec, any_spec],
        out_specs=[any_spec] * 3,
        scratch_shapes=[
            V((HP, HP, NB, CIN), BF), V((HP, HP, NB, LN), BF), V((TAPS, CIN, BLK), BF), V((4, TAPS, BLK, BLK), BF), V((4, 2304, BLK), BF),
            V((HW, HW, NB, BLK), BF), V((4, HP, HP, NB, BLK), BF), V((4, TAPS, LN, BLK), F32), V((4, TAPS, LN, BLK), F32),
            V((14, RW, BLK), F32), V((14, HW, NB, BLK), BF), V((7, HW, 2, CIN), BF),
            D((2,)), D((3,)), D((3,)), D((3,)), D((3,)), D((3,)), D((3,)), D((6,)), D((6,)), D((6,)), D((CH,)), D((2,)), D((2,)), D((2,)), D((4, CH)), D((3, CH)), D((1,)), D((1,)),
            D((2, CH)), D((2, CH)), D((3, GX)), D((3, GX)), D((2, CH)), D((2, CH)), D((5,)), D((5,)), D((3, 4)), D((3, 4)), D((4, 7)), D((4, 7)), D((5,)),
        ],
        compiler_params=pltpu.CompilerParams(collective_id=0, has_side_effects=True, vmem_limit_bytes=66000000),
        name="conv_block",
    )

    def body(act_loc, w_loc, scale_loc, shift_loc, grad_loc):
        z, da, dw = call(act_loc[0].transpose(1, 2, 0, 3), w_loc[0].reshape(TAPS, LN, 1024), scale_loc, shift_loc, grad_loc[0].transpose(1, 2, 0, 3))
        z = jnp.maximum(z, 0.0)
        return z.transpose(2, 0, 1, 3)[None], da.transpose(2, 0, 1, 3)[None], dw.reshape(1, 3, 3, LN, 1024)

    act_spec = P("stage", ("dp", "tp"))
    w_spec = P("stage", None, None, "tp")
    vec_spec = P("stage", "tp")
    grad_spec = P("stage", "dp", None, None, "tp")
    return jax.shard_map(body, mesh=mesh, in_specs=(act_spec, w_spec, vec_spec, vec_spec, grad_spec), out_specs=(grad_spec, act_spec, w_spec), check_vma=False)
```
